32 devices in a mesh: row: 4 (over y, x), col: 8 (over z, core).
Axes of the slice: x: 2, y: 2, z: 4, core: 2. Of those that a mesh axis runs over, the one named last changes fastest.
Arguments:
- features: bfloat16 [32768, 128], P(('row', 'col')), may hold values from -24 to 24
- tile_rows: int32 [4, 8, 1024], P('row', 'col'), may hold values from 0 to 63
- tile_cols: int32 [4, 8, 1024], P('row', 'col'), may hold values from 0 to 31
- edge_lists: int32 [2, 4, 8, 1024, 128], P(None, 'row', 'col'), may hold values from -16 to 127
- tile_counts: int32 [4, 8], P('row', 'col'), may hold values from 128 to 1024, as said below
Outputs:
- hop_one: bfloat16 [32768, 128], P(('row', 'col'))
- hop_two: bfloat16 [32768, 128], P(('row', 'col'))
The draws below stay inside these ranges and needn't reach their ends.
Inputs may be any that keep to these rules, and one draw needn't show every extreme that they name: `tile_counts`: live tile slots of a block; some block has exactly 1024. `edge_lists`: a negative entry marks an empty edge slot; slots at or past a block's count hold arbitrary entries. `tile_rows`: a tile may occur in several slots; slots at or past a block's count hold arbitrary entries. `tile_cols`: slots at or past a block's count hold arbitrary entries.
All inputs are finite; a program needn't handle non-finite values.
Results may differ from the reference program's by a relative error of at most 0.0058.
Values may be sent and summed in bfloat16 or wider, within the bound.
A program may use at most 192 MiB of HBM per device.

```python
import jax
import jax.numpy as jnp
from jax import lax

F = 128
TILE = 128
EDGE_TILE = 128
NODE_DEV = 1024
TILE_MOST = 1024
NODES = 32768
TILE_ROWS = 64
TILE_COLS = 32
N_ROW = 4
N_COL = 8


def draw_tile_counts(key, part):
    base = jax.random.randint(jax.random.fold_in(key, 11), (N_ROW * N_COL,), TILE_MOST // 8, TILE_MOST // 2 + 1)
    busiest = jax.random.randint(jax.random.fold_in(key, 12), (), 0, N_ROW * N_COL)
    placed = jnp.where(jnp.arange(N_ROW * N_COL) == busiest, TILE_MOST, base)
    return placed.reshape(N_ROW, N_COL).astype(jnp.int32)


def set_ends(result, key, smallest, high):
    shape = result.shape
    place = [jax.random.randint(jax.random.fold_in(key, axis), (), 0, shape[axis]) for axis in range(len(shape))]
    result = result.at[tuple(place)].set(smallest)
    longest = shape.index(max(shape))
    place[longest] = (place[longest] + 1) % shape[longest]
    return result.at[tuple(place)].set(high)


def level_of(key, dims, shards, low, largest):
    factor_of, own = 1.0, jax.random.fold_in(key, 6)
    for dim, shards_of in shards:
        steps = jnp.exp(jax.random.uniform(jax.random.fold_in(own, dim), (shards_of,), jnp.float32, low / len(shards), largest / len(shards)))
        factor_of = factor_of * jnp.repeat(steps, dims[dim] // shards_of).reshape([-1 if axis == dim else 1 for axis in range(len(dims))])
    return factor_of


def scatter_about(rng, shape, scale, bound, shards=(), dtype=jnp.bfloat16):
    values = scale * jax.random.normal(rng, shape, jnp.float32)
    if shards:
        values = values * level_of(rng, shape, shards, -0.22, 0.18)
    return jnp.clip(values, -bound, bound).astype(dtype)


def setup_inputs(seed: int = 0) -> dict:
    keys = jax.random.split(jax.random.key(seed), 6)
    features = scatter_about(keys[0], (NODES, F), 4.0, 24.0, ((0, 32),))
    tile_rows = set_ends(jax.random.randint(keys[1], (N_ROW, N_COL, TILE_MOST), 0, TILE_ROWS), jax.random.fold_in(keys[1], 1), 0, TILE_ROWS - 1).astype(jnp.int32)
    tile_cols = set_ends(jax.random.randint(keys[2], (N_ROW, N_COL, TILE_MOST), 0, TILE_COLS), jax.random.fold_in(keys[2], 1), 0, TILE_COLS - 1).astype(jnp.int32)
    edge_lists = set_ends(jax.random.randint(keys[3], (2, N_ROW, N_COL, TILE_MOST, EDGE_TILE), -16, TILE), jax.random.fold_in(keys[3], 1), -16, TILE - 1).astype(jnp.int32)
    tile_counts = draw_tile_counts(jax.random.fold_in(keys[5], 71), 0)
    return dict(features=features, tile_rows=tile_rows, tile_cols=tile_cols, edge_lists=edge_lists, tile_counts=tile_counts)


def reference(features, tile_rows, tile_cols, edge_lists, tile_counts):
    node_total = NODE_DEV * N_ROW * N_COL
    block_nodes = NODE_DEV * N_COL
    slot_ids = lax.iota(jnp.int32, TILE_MOST)

    def edges_of(device_idx):
        row_idx = device_idx // N_COL
        col_idx = device_idx % N_COL
        dst_ids = edge_lists[0, row_idx, col_idx]
        src_ids = edge_lists[1, row_idx, col_idx]
        alive = (slot_ids < tile_counts[row_idx, col_idx])[:, None] & (dst_ids >= 0) & (src_ids >= 0)
        target = row_idx * block_nodes + tile_rows[row_idx, col_idx][:, None] * TILE + dst_ids
        column = tile_cols[row_idx, col_idx][:, None] * TILE + src_ids
        source = (column // NODE_DEV * N_COL + col_idx) * NODE_DEV + column % NODE_DEV
        target = jnp.where(alive, target, 0).reshape(-1)
        source = jnp.where(alive, source, 0).reshape(-1)
        return (target, source, alive.astype(jnp.float32).reshape(-1))

    def count_edges(device_idx, degree):
        target, source, weight = edges_of(device_idx)
        return degree.at[target].add(weight)
    degree = lax.fori_loop(0, N_ROW * N_COL, count_edges, jnp.zeros((node_total,), jnp.float32))
    inv_root = lax.rsqrt(1.0 + degree)

    def propagate(scaled):

        def add_edges(device_idx, summed):
            target, source, weight = edges_of(device_idx)
            return summed.at[target].add(scaled[source].astype(jnp.float32) * weight[:, None])
        return lax.fori_loop(0, N_ROW * N_COL, add_edges, jnp.zeros((node_total, F), jnp.float32))
    scaled_zero = (features.astype(jnp.float32) * inv_root[:, None]).astype(jnp.bfloat16)
    first_sum = propagate(scaled_zero)
    hop_one = (first_sum * inv_root[:, None]).astype(jnp.bfloat16)
    scaled_one = (first_sum * (inv_root * inv_root)[:, None]).astype(jnp.bfloat16)
    second_sum = propagate(scaled_one)
    hop_two = (second_sum * inv_root[:, None]).astype(jnp.bfloat16)
    return (hop_one, hop_two)
```

```python
import functools

import jax
import jax.numpy as jnp
from jax import lax
from jax.experimental import pallas as pl
from jax.experimental.pallas import tpu as pltpu
from jax.sharding import PartitionSpec as P

TILE = 128
ROWS_MIN = 16
BUILD_UNROLL = 32
APPLY_UNROLL = 32
APPLY_SLOTS = 4
HOT = jnp.float8_e4m3fn
HOT_EXTRA = 32
EXTRA = 16
PIECES = 4
CORES = 2
MESH_ID = pl.DeviceIdType.MESH
VMEM_SPEC = pl.BlockSpec(memory_space=pltpu.VMEM)
SMEM_SPEC = pl.BlockSpec(memory_space=pltpu.SMEM)
ANY_SPEC = pl.BlockSpec(memory_space=pl.ANY)


def place_of():
    row, col = lax.axis_index("row"), lax.axis_index("col")
    return row, col, lax.rem(col, CORES), col // CORES


def order_kernel(own, n_chip, count_ref, rows_ref, cols_ref, order_ref):
    slots = rows_ref.shape[-1]
    places = order_ref.shape[-1]
    bins = CORES * n_chip * own
    bf16, f32 = jnp.bfloat16, jnp.float32
    _, _, core, chip = place_of()

    def iota(shape, dim):
        return lax.broadcasted_iota(jnp.int32, shape, dim)

    def hot(mask):
        return jnp.where(mask, 1.0, 0.0).astype(bf16)

    def mul(x, y):
        return jnp.dot(x.astype(bf16), y.astype(bf16), preferred_element_type=f32)

    slot = iota((1, slots), 1)
    alive = slot < count_ref[0]
    rows = jnp.where(alive, rows_ref[...], 0)
    cols = jnp.where(alive, cols_ref[...], 0)
    owner = rows // own
    target = owner // CORES
    other = jnp.where(lax.rem(owner, CORES) == core, 0, 1)
    rank = jnp.where(chip < n_chip // 2, n_chip - 1 - target, target)
    within = lax.rem(rows, own)
    bin_of = jnp.where(alive, (other * n_chip + rank) * own + within, -1)
    local = target * own + within
    belongs = bin_of == iota((bins, slots), 0)
    ranks = mul(hot(belongs), hot(iota((slots, slots), 0) <= iota((slots, slots), 1)))
    totals = jnp.broadcast_to(ranks[:, slots - 1 :], (bins, TILE)).astype(jnp.int32)
    pairs = (totals + 1) // 2
    before = hot(iota((bins, bins), 1) < iota((bins, bins), 0))
    offsets = 2.0 * (
        32.0 * mul(before, (pairs // 32).astype(f32)) + mul(before, (pairs % 32).astype(f32))
    )
    spots = jnp.where(belongs, ranks - 1.0 + offsets[:, :1], 0.0)
    spot = jnp.where(alive, jnp.sum(spots, axis=0, keepdims=True), -1.0)
    spot = jnp.broadcast_to(spot, (TILE, slots)).T.astype(jnp.int32)
    facts = [slot // 32, slot % 32, jnp.where(alive, 1, 0), local, cols]
    facts = jnp.concatenate(
        [fact.astype(f32) for fact in facts] + [jnp.zeros((EXTRA - len(facts), slots), f32)], axis=0
    )
    for block in range(places // TILE):
        taken = hot(spot == iota((slots, TILE), 1) + block * TILE)
        found = mul(facts, taken).astype(jnp.int32)
        place = 32 * found[0:1] + found[1:2] + found[2:3] - 1
        order_ref[:, block * TILE : (block + 1) * TILE] = jnp.concatenate(
            [place, found[3:5], jnp.zeros((5, TILE), jnp.int32)], axis=0
        )
    order_ref[3:4, 0:bins] = offsets.T[0:1, :].astype(jnp.int32)
    end = jnp.sum(2.0 * pairs.astype(f32), axis=0, keepdims=True).astype(jnp.int32)
    order_ref[4:5, 0:TILE] = end


def span_of(order_ref, half_bins, other):
    middle = order_ref[3, half_bins]
    if other:
        return middle, order_ref[4, 0]
    return 0, middle


def build_kernel(half_bins, other, order_ref, dst_ref, src_ref, store_ref, degree_ref, made, degree_acc, sem):
    degree_acc[...] = jnp.zeros_like(degree_acc)
    low, high = span_of(order_ref, half_bins, other)
    turns = (high - low + BUILD_UNROLL - 1) // BUILD_UNROLL
    pairs = BUILD_UNROLL // 2
    cells = lax.broadcasted_iota(jnp.int32, (TILE, TILE), 0)

    def out_copy(turn):
        side = lax.rem(turn, 2)
        return pltpu.make_async_copy(
            made.at[side], store_ref.at[pl.ds(turn * pairs, pairs)], sem.at[side]
        )

    def visit(turn, carry):
        side = lax.rem(turn, 2)

        @pl.when(turn >= 2)
        def _():
            out_copy(turn - 2).wait()

        for pair in range(pairs):
            counts = []
            base = low + turn * BUILD_UNROLL + 2 * pair
            for half in range(2):
                slot = jnp.where(base < high, order_ref[0, base + half], -1)
                safe = jnp.maximum(slot, 0)
                dst = jnp.where(slot >= 0, dst_ref[pl.ds(safe, 1), :], -1)
                src = src_ref[pl.ds(safe, 1), :]
                dst_hot = jnp.where(dst == cells, 1.0, 0.0).astype(HOT)
                src_hot = jnp.where(src == cells, 1.0, 0.0).astype(HOT)
                valid = jnp.broadcast_to(jnp.where(src >= 0, 1.0, 0.0), (HOT_EXTRA, TILE))
                left = jnp.concatenate([src_hot, valid.astype(HOT)], axis=0)
                both = lax.dot_general(
                    left, dst_hot, (((1,), (1,)), ((), ())), preferred_element_type=jnp.float32
                )
                made[side, pair, half * TILE : (half + 1) * TILE] = both[:TILE].astype(jnp.bfloat16)
                counts.append(both[TILE : TILE + 8])
            degree_acc[order_ref[1, base]] += counts[0] + counts[1]
        out_copy(turn).start()
        return carry

    lax.fori_loop(0, turns, visit, 0)

    @pl.when(turns >= 2)
    def _():
        out_copy(turns - 2).wait()

    @pl.when(turns >= 1)
    def _():
        out_copy(turns - 1).wait()

    degree_ref[...] = degree_acc[:, 0, :]


def apply_kernel(half_bins, orders, stores, source_ref, out_ref, held, acc, sem):
    acc[...] = jnp.zeros_like(acc)
    pairs = APPLY_UNROLL // 2
    spans = [span_of(order, half_bins, other) for other, order in enumerate(orders)]
    turns = [(high - low + APPLY_UNROLL - 1) // APPLY_UNROLL for low, high in spans]
    total = turns[0] + turns[1]

    def fetch(turn):
        slot = lax.rem(turn, APPLY_SLOTS)
        for other in range(2):
            local = turn - other * turns[0]

            @pl.when((local >= 0) & (local < turns[other]))
            def _():
                pltpu.make_async_copy(
                    stores[other].at[pl.ds(local * pairs, pairs)], held.at[slot], sem.at[slot]
                ).start()

    for turn in range(APPLY_SLOTS - 1):
        fetch(turn)

    for other in range(2):
        order_ref = orders[other]
        low, high = spans[other]
        offset = other * source_ref.shape[0] // 2

        def visit(turn, carry):
            slot = lax.rem(turn, APPLY_SLOTS)
            pltpu.make_async_copy(
                stores[0].at[pl.ds(0, pairs)], held.at[slot], sem.at[slot]
            ).wait()
            fetch(turn + APPLY_SLOTS - 1)
            for pair in range(pairs):
                base = low + (turn - other * turns[0]) * APPLY_UNROLL + 2 * pair
                sources = jnp.concatenate(
                    [
                        source_ref[offset + order_ref[2, base]],
                        source_ref[offset + order_ref[2, base + 1]],
                    ],
                    axis=1,
                )
                acc[order_ref[1, base]] += jnp.dot(
                    sources, held[slot, pair], preferred_element_type=jnp.float32
                )
            return carry

        lax.fori_loop(other * turns[0], turns[0] + other * turns[1], visit, 0)
    out_ref[...] = acc[...].astype(jnp.bfloat16)


def greet(targets):
    barrier = pltpu.get_barrier_semaphore()
    for target in targets:
        pl.semaphore_signal(barrier, inc=1, device_id=target, device_id_type=MESH_ID)
    pl.semaphore_wait(barrier, len(targets))


def row_peers(n_row, side=0):
    row, col, core, chip = place_of()
    if side:
        col = chip * CORES + 1 - core
    return [(lax.rem(row + d, n_row), col) for d in range(1, n_row)]


def sibling_peers(n_col):
    row, col, _, _ = place_of()
    return [(row, lax.rem(col + CORES * d, n_col)) for d in range(1, n_col // CORES)]


def partner_of():
    row, col, core, chip = place_of()
    return (row, chip * CORES + 1 - core)


def remote(src, dst, send_sem, recv_sem, target):
    return pltpu.make_async_remote_copy(
        src_ref=src,
        dst_ref=dst,
        send_sem=send_sem,
        recv_sem=recv_sem,
        device_id=target,
        device_id_type=MESH_ID,
    )


def send(*args):
    copy = remote(*args)
    copy.start()
    return copy


def prep_kernel(features_ref, out_ref):
    for tile in range(out_ref.shape[0]):
        block = features_ref[tile * TILE : (tile + 1) * TILE, :].astype(jnp.float32).T
        out_ref[tile] = block.astype(jnp.bfloat16)


def start_kernel(n_row, n_col, deg_a_ref, deg_b_ref, *refs):
    blocks = refs[:n_row]
    gathered_ref, root_ref, part, taken, theirs, roots = refs[n_row : n_row + 6]
    deg_send, deg_recv, near_send, near_recv, root_send, root_recv = refs[n_row + 6 :]
    row, col, core, chip = place_of()
    n_chip = n_col // CORES
    own = root_ref.shape[0]
    partner = partner_of()
    siblings = sibling_peers(n_col)
    mine, cross = row_peers(n_row), row_peers(n_row, 1)
    greet(siblings + mine + cross + [partner])
    part[...] = deg_a_ref[...] + deg_b_ref[...]
    copies = []
    for d, target in enumerate(siblings):
        start = (target[1] // CORES) * own
        copies.append(
            send(
                part.at[pl.ds(pl.multiple_of(start, own), own)],
                taken.at[d],
                deg_send.at[d],
                deg_recv.at[d],
                target,
            )
        )
    near = []
    for d in range(n_row):
        near.append(send(blocks[d], theirs.at[d], near_send.at[d], near_recv.at[d], partner))
    degree = part[pl.ds(pl.multiple_of(chip * own, own), own), :]
    for d, copy in enumerate(copies):
        copy.wait_recv()
        degree = degree + taken[d]
    root = lax.rsqrt(1.0 + degree)
    root_ref[...] = root
    roots[0, 0] = root
    root_copies = []
    for side, targets in ((0, mine), (1, [partner] + cross)):
        for d, target in enumerate(targets):
            d += 1 - side
            root_copies.append(
                send(roots.at[0, 0], roots.at[side, d], root_send.at[side, d], root_recv.at[side, d], target)
            )

    def scale(side, d, source, root):
        start = side * n_row * own + lax.rem(row + n_row - d, n_row) * own
        for tile in range(own):
            gathered_ref[start + tile] = (
                source[tile].astype(jnp.float32) * root[tile : tile + 1, :]
            ).astype(jnp.bfloat16)

    scale(0, 0, blocks[0], root)
    for copy in root_copies:
        copy.wait_recv()
    for d in range(1, n_row):
        scale(0, d, blocks[d], roots[0, d])
    for d in range(n_row):
        near[d].wait_recv()
        scale(1, d, theirs.at[d], roots[1, d])
    for copy in copies + near + root_copies:
        copy.wait_send()


def sum_kernel(n_row, n_col, spread, part_ref, root_ref, *refs):
    if spread:
        hop_ref, gathered_ref, comes, goes, *sems = refs
        send_sem, recv_sem, row_send, row_recv, near_send, near_recv = sems
    else:
        hop_ref, comes, goes, send_sem, recv_sem = refs
    row, col, core, chip = place_of()
    n_chip = n_col // CORES
    own = root_ref.shape[0]
    size = own // PIECES
    partner = partner_of()
    up = (row, lax.rem(col + CORES, n_col))
    down = (row, lax.rem(col + n_col - CORES, n_col))
    mine = row_peers(n_row)
    greet([up, down] + ([partner] + mine if spread else []))
    last = n_chip - 1

    def hop_copy(way, k, piece, direct):
        target = last - k if way == 0 else k
        source = (
            part_ref.at[pl.ds(target * own + piece * size, size)] if direct else goes.at[way, k, piece]
        )
        return remote(
            source,
            comes.at[way, k, piece],
            send_sem.at[way, k, piece],
            recv_sem.at[way, k, piece],
            down if way else up,
        )

    def steps():
        for k in range(last):
            for piece in range(PIECES):
                for way in range(2):
                    target = last - k if way == 0 else k
                    ahead = (chip < target) if way == 0 else (chip > target)
                    first = chip == (0 if way == 0 else last)
                    yield k, piece, way, target, ahead, first

    for k, piece, way, target, ahead, first in steps():

        @pl.when(ahead & first)
        def _():
            hop_copy(way, k, piece, True).start()

        @pl.when(ahead & jnp.logical_not(first))
        def _():
            hop_copy(way, k, piece, False).wait_recv()
            start = target * own + piece * size
            goes[way, k, piece] = (
                part_ref[start : start + size].astype(jnp.float32)
                + comes[way, k, piece].astype(jnp.float32)
            ).astype(jnp.bfloat16)
            hop_copy(way, k, piece, False).start()

    row_copies, near_copies = {}, {}
    for piece in range(PIECES):
        for way, k, fed in ((0, last - chip, chip > 0), (1, chip, chip < last)):

            @pl.when(fed)
            def _():
                hop_copy(way, k, piece, False).wait_recv()

        total = part_ref[pl.ds(chip * own + piece * size, size)].astype(jnp.float32)
        below = comes[0, jnp.minimum(last - chip, last - 1), piece].astype(jnp.float32)
        above = comes[1, jnp.minimum(chip, last - 1), piece].astype(jnp.float32)
        total = total + jnp.where(chip > 0, below, 0.0) + jnp.where(chip < last, above, 0.0)
        roots = [root_ref[piece * size + tile : piece * size + tile + 1, :] for tile in range(size)]
        if spread:
            start = row * own + piece * size
            for tile in range(size):
                gathered_ref[start + tile] = (total[tile] * (roots[tile] * roots[tile])).astype(
                    jnp.bfloat16
                )
            for d, target in enumerate(mine):
                place = gathered_ref.at[pl.ds(start, size)]
                row_copies[piece, d] = send(
                    place, place, row_send.at[piece, d], row_recv.at[piece, d], target
                )
            near_copies[piece, 0] = send(
                gathered_ref.at[pl.ds(start, size)],
                gathered_ref.at[pl.ds(n_row * own + start, size)],
                near_send.at[piece, 0],
                near_recv.at[piece, 0],
                partner,
            )
        for tile in range(size):
            place = (piece * size + tile) * TILE
            hop_ref[place : place + TILE, :] = (total[tile] * roots[tile]).T.astype(jnp.bfloat16)
    for (piece, d), copy in row_copies.items():
        copy.wait_recv()
        start = lax.rem(row + n_row - d - 1, n_row) * own + piece * size
        near_copies[piece, d + 1] = send(
            gathered_ref.at[pl.ds(start, size)],
            gathered_ref.at[pl.ds(n_row * own + start, size)],
            near_send.at[piece, d + 1],
            near_recv.at[piece, d + 1],
            partner,
        )
    for copy in near_copies.values():
        copy.wait_recv()
    for copy in list(row_copies.values()) + list(near_copies.values()):
        copy.wait_send()
    for k, piece, way, target, ahead, first in steps():

        @pl.when(ahead)
        def _():
            hop_copy(way, k, piece, False).wait_send()


def sems(*shape):
    return pltpu.SemaphoreType.DMA(shape)


def comm_params(ident):
    return pltpu.CompilerParams(
        collective_id=ident, has_side_effects=True, vmem_limit_bytes=48 * 2**20
    )


def plain_params():
    return pltpu.CompilerParams(vmem_limit_bytes=48 * 2**20)


def local(features, tile_rows, tile_cols, edge_lists, tile_counts):
    node_count, feat_width = features.shape
    n_row, n_col = lax.axis_size("row"), lax.axis_size("col")
    n_chip = n_col // CORES
    own = node_count // TILE
    half_tiles = own * n_chip
    source_tiles = own * n_row
    slots = tile_rows.shape[-1]
    bf16, f32 = jnp.bfloat16, jnp.float32
    places = -(-(slots + CORES * half_tiles) // TILE) * TILE
    swap = [(i, i + 1 - 2 * (i % CORES)) for i in range(n_col)]

    edges_b = lax.ppermute(edge_lists, "col", swap)
    own_type = jax.ShapeDtypeStruct((own, feat_width, TILE), bf16)
    turned = pl.pallas_call(
        prep_kernel,
        out_shape=own_type,
        in_specs=[VMEM_SPEC],
        out_specs=VMEM_SPEC,
        name="prep",
    )(features)
    blocks = [turned] + [
        lax.ppermute(turned, "row", [(i, (i + d) % n_row) for i in range(n_row)])
        for d in range(1, n_row)
    ]

    order = pl.pallas_call(
        functools.partial(order_kernel, own, n_chip),
        out_shape=jax.ShapeDtypeStruct((8, places), jnp.int32),
        in_specs=[SMEM_SPEC, VMEM_SPEC, VMEM_SPEC],
        out_specs=VMEM_SPEC,
        compiler_params=plain_params(),
        name="order",
    )(tile_counts[0], tile_rows[0], tile_cols[0])
    order_b = lax.ppermute(order, "col", swap)

    def build(order, edges, other):
        edges = edges.reshape(2, slots, TILE)
        return pl.pallas_call(
            functools.partial(build_kernel, half_tiles, other),
            in_specs=[SMEM_SPEC]
            + [
                pl.BlockSpec((None, slots, TILE), lambda i, side=side: (side, 0, 0))
                for side in range(2)
            ],
            grid=(1,),
            out_specs=[ANY_SPEC, pl.BlockSpec((half_tiles, TILE), lambda i: (0, 0))],
            scratch_shapes=[
                pltpu.VMEM((2, BUILD_UNROLL // 2, 2 * TILE, TILE), bf16),
                pltpu.VMEM((half_tiles, 8, TILE), f32),
                sems(2),
            ],
            out_shape=[
                jax.ShapeDtypeStruct((places // 2, 2 * TILE, TILE), bf16),
                jax.ShapeDtypeStruct((half_tiles, TILE), f32),
            ],
            compiler_params=plain_params(),
            cost_estimate=pl.CostEstimate(flops=10**10, bytes_accessed=0, transcendentals=0),
            name="build",
        )(order, edges, edges)

    store_a, degree_a = build(order, edge_lists, False)
    store_b, degree_b = build(order_b, edges_b, True)

    gathered_type = jax.ShapeDtypeStruct((CORES * source_tiles, feat_width, TILE), bf16)
    gathered, root = pl.pallas_call(
        functools.partial(start_kernel, n_row, n_col),
        out_shape=[gathered_type, jax.ShapeDtypeStruct((own, TILE), f32)],
        in_specs=[VMEM_SPEC] * (2 + n_row),
        out_specs=[VMEM_SPEC] * 2,
        scratch_shapes=[
            pltpu.VMEM((half_tiles, TILE), f32),
            pltpu.VMEM((n_chip - 1, own, TILE), f32),
            pltpu.VMEM((n_row, own, feat_width, TILE), bf16),
            pltpu.VMEM((2, n_row, own, TILE), f32),
            sems(n_chip - 1),
            sems(n_chip - 1),
            sems(n_row),
            sems(n_row),
            sems(2, n_row),
            sems(2, n_row),
        ],
        compiler_params=comm_params(0),
        name="start",
    )(degree_a, degree_b, *blocks)

    def apply(sources):
        def body(order_a, order_b, store_a, store_b, *refs):
            apply_kernel(half_tiles, (order_a, order_b), (store_a, store_b), *refs)

        return pl.pallas_call(
            body,
            in_specs=[SMEM_SPEC] * 2 + [ANY_SPEC] * 2 + [VMEM_SPEC],
            out_specs=VMEM_SPEC,
            scratch_shapes=[
                pltpu.VMEM((APPLY_SLOTS, APPLY_UNROLL // 2, 2 * TILE, TILE), bf16),
                pltpu.VMEM((half_tiles, feat_width, TILE), f32),
                sems(APPLY_SLOTS),
            ],
            out_shape=jax.ShapeDtypeStruct((half_tiles, feat_width, TILE), bf16),
            compiler_params=plain_params(),
            name="apply",
        )(order, order_b, store_a, store_b, sources)

    def collect(part, spread):
        size = own // PIECES
        outs = [jax.ShapeDtypeStruct((node_count, feat_width), bf16)]
        semaphores = [sems(2, n_chip - 1, PIECES)] * 2
        if spread:
            outs.append(gathered_type)
            semaphores += [sems(PIECES, n_row - 1)] * 2 + [sems(PIECES, n_row)] * 2
        return pl.pallas_call(
            functools.partial(sum_kernel, n_row, n_col, spread),
            out_shape=outs,
            in_specs=[VMEM_SPEC] * 2,
            out_specs=[VMEM_SPEC] * len(outs),
            scratch_shapes=[pltpu.VMEM((2, n_chip - 1, PIECES, size, feat_width, TILE), bf16)] * 2
            + semaphores,
            compiler_params=comm_params(1 if spread else 2),
            name="spread" if spread else "finish",
        )(part, root)

    hop_one, gathered = collect(apply(gathered), True)
    (hop_two,) = collect(apply(gathered), False)
    return (hop_one, hop_two)


def solution(mesh):
    placed = (
        P(("row", "col"), None),
        P("row", "col", None),
        P("row", "col", None),
        P(None, "row", "col", None, None),
        P("row", "col"),
    )
    return jax.shard_map(
        local,
        mesh=mesh,
        in_specs=placed,
        out_specs=(P(("row", "col"), None), P(("row", "col"), None)),
        check_vma=False,
    )
```

```python
import functools

import jax
import jax.numpy as jnp
from jax import lax
from jax.experimental import pallas as pl
from jax.experimental.pallas import tpu as pltpu
from jax.sharding import PartitionSpec as P

TILE = 128
ROWS_MIN = 16
BUILD_UNROLL = 32
APPLY_UNROLL = 32
APPLY_SLOTS = 4
HOT = jnp.float8_e4m3fn
HOT_ROWS = 32
EXTRA = 16
PIECES = 4
RELAY_LAG = 3
CORES = 2
MESH_ID = pl.DeviceIdType.MESH
VMEM_SPEC = pl.BlockSpec(memory_space=pltpu.VMEM)
SMEM_SPEC = pl.BlockSpec(memory_space=pltpu.SMEM)
ANY_SPEC = pl.BlockSpec(memory_space=pl.ANY)


def place_of():
    row, col = lax.axis_index("row"), lax.axis_index("col")
    return row, col, lax.rem(col, CORES), col // CORES


def order_kernel(own, n_chip, count_ref, rows_ref, cols_ref, order_ref):
    slots = rows_ref.shape[-1]
    places = order_ref.shape[-1]
    bins = CORES * n_chip * own
    bf16, f32 = jnp.bfloat16, jnp.float32
    _, _, core, chip = place_of()

    def iota(shape, dim):
        return lax.broadcasted_iota(jnp.int32, shape, dim)

    def hot(mask):
        return jnp.where(mask, 1.0, 0.0).astype(bf16)

    def mul(x, y):
        return jnp.dot(x.astype(bf16), y.astype(bf16), preferred_element_type=f32)

    slot = iota((1, slots), 1)
    alive = slot < count_ref[0]
    rows = jnp.where(alive, rows_ref[...], 0)
    cols = jnp.where(alive, cols_ref[...], 0)
    owner = rows // own
    target = owner // CORES
    other = jnp.where(lax.rem(owner, CORES) == core, 0, 1)
    rank = jnp.where(chip < n_chip // 2, n_chip - 1 - target, target)
    within = lax.rem(rows, own)
    bin_of = jnp.where(alive, (other * n_chip + rank) * own + within, -1)
    local = target * own + within
    belongs = bin_of == iota((bins, slots), 0)
    ranks = mul(hot(belongs), hot(iota((slots, slots), 0) <= iota((slots, slots), 1)))
    totals = jnp.broadcast_to(ranks[:, slots - 1 :], (bins, TILE)).astype(jnp.int32)
    pairs = (totals + 1) // 2
    before = hot(iota((bins, bins), 1) < iota((bins, bins), 0))
    offsets = 2.0 * (
        32.0 * mul(before, (pairs // 32).astype(f32)) + mul(before, (pairs % 32).astype(f32))
    )
    spots = jnp.where(belongs, ranks - 1.0 + offsets[:, :1], 0.0)
    spot = jnp.where(alive, jnp.sum(spots, axis=0, keepdims=True), -1.0)
    spot = jnp.broadcast_to(spot, (TILE, slots)).T.astype(jnp.int32)
    facts = [slot // 32, slot % 32, jnp.where(alive, 1, 0), local, cols]
    facts = jnp.concatenate(
        [fact.astype(f32) for fact in facts] + [jnp.zeros((EXTRA - len(facts), slots), f32)], axis=0
    )
    for block in range(places // TILE):
        taken = hot(spot == iota((slots, TILE), 1) + block * TILE)
        found = mul(facts, taken).astype(jnp.int32)
        place = 32 * found[0:1] + found[1:2] + found[2:3] - 1
        order_ref[:, block * TILE : (block + 1) * TILE] = jnp.concatenate(
            [place, found[3:5], jnp.zeros((5, TILE), jnp.int32)], axis=0
        )
    order_ref[3:4, 0:bins] = offsets.T[0:1, :].astype(jnp.int32)
    end = jnp.sum(2.0 * pairs.astype(f32), axis=0, keepdims=True).astype(jnp.int32)
    order_ref[4:5, 0:TILE] = end


def span_of(order_ref, half_bins, other):
    middle = order_ref[3, half_bins]
    if other:
        return middle, order_ref[4, 0]
    return 0, middle


def build_kernel(half_bins, other, order_ref, dst_ref, src_ref, store_ref, degree_ref, made, degree_acc, sem):
    degree_acc[...] = jnp.zeros_like(degree_acc)
    low, high = span_of(order_ref, half_bins, other)
    turns = (high - low + BUILD_UNROLL - 1) // BUILD_UNROLL
    pairs = BUILD_UNROLL // 2
    cells = [
        (lax.broadcasted_iota(jnp.int32, (HOT_ROWS, TILE), 0) + start).astype(jnp.int8)
        for start in range(0, TILE, HOT_ROWS)
    ]

    def hot(ids):
        ids = jnp.broadcast_to(ids, (HOT_ROWS, TILE)).astype(jnp.int8)
        return jnp.concatenate(
            [jnp.where(ids == cell, HOT(1), HOT(0)) for cell in cells], axis=0
        )

    def out_copy(turn):
        side = lax.rem(turn, 2)
        return pltpu.make_async_copy(
            made.at[side], store_ref.at[pl.ds(turn * pairs, pairs)], sem.at[side]
        )

    def visit(turn, carry):
        side = lax.rem(turn, 2)

        @pl.when(turn >= 2)
        def _():
            out_copy(turn - 2).wait()

        for pair in range(pairs):
            counts = []
            base = low + turn * BUILD_UNROLL + 2 * pair
            for half in range(2):
                slot = jnp.where(base < high, order_ref[0, base + half], -1)
                safe = jnp.maximum(slot, 0)
                dst = jnp.where(slot >= 0, dst_ref[pl.ds(safe, 1), :], -1)
                src = src_ref[pl.ds(safe, 1), :]
                both = lax.dot_general(
                    hot(src), hot(dst), (((1,), (1,)), ((), ())), preferred_element_type=jnp.float32
                )
                made[side, pair, half * TILE : (half + 1) * TILE] = both.astype(jnp.bfloat16)
                counts.append(jnp.sum(both.reshape(TILE // 8, 8, TILE), axis=0))
            degree_acc[order_ref[1, base]] += counts[0] + counts[1]
        out_copy(turn).start()
        return carry

    lax.fori_loop(0, turns, visit, 0)

    @pl.when(turns >= 2)
    def _():
        out_copy(turns - 2).wait()

    @pl.when(turns >= 1)
    def _():
        out_copy(turns - 1).wait()

    degree_ref[...] = jnp.sum(degree_acc[...], axis=1)


def apply_kernel(half_bins, orders, stores, source_ref, out_ref, held, acc, sem):
    acc[...] = jnp.zeros_like(acc)
    pairs = APPLY_UNROLL // 2
    spans = [span_of(order, half_bins, other) for other, order in enumerate(orders)]
    turns = [(high - low + APPLY_UNROLL - 1) // APPLY_UNROLL for low, high in spans]
    total = turns[0] + turns[1]

    def fetch(turn):
        slot = lax.rem(turn, APPLY_SLOTS)
        for other in range(2):
            local = turn - other * turns[0]

            @pl.when((local >= 0) & (local < turns[other]))
            def _():
                pltpu.make_async_copy(
                    stores[other].at[pl.ds(local * pairs, pairs)], held.at[slot], sem.at[slot]
                ).start()

    for turn in range(APPLY_SLOTS - 1):
        fetch(turn)

    for other in range(2):
        order_ref = orders[other]
        low, high = spans[other]
        offset = other * source_ref.shape[0] // 2

        def visit(turn, carry):
            slot = lax.rem(turn, APPLY_SLOTS)
            pltpu.make_async_copy(
                stores[0].at[pl.ds(0, pairs)], held.at[slot], sem.at[slot]
            ).wait()
            fetch(turn + APPLY_SLOTS - 1)
            for pair in range(pairs):
                base = low + (turn - other * turns[0]) * APPLY_UNROLL + 2 * pair
                sources = jnp.concatenate(
                    [
                        source_ref[offset + order_ref[2, base]],
                        source_ref[offset + order_ref[2, base + 1]],
                    ],
                    axis=1,
                )
                acc[order_ref[1, base]] += jnp.dot(
                    sources, held[slot, pair], preferred_element_type=jnp.float32
                )
            return carry

        lax.fori_loop(other * turns[0], turns[0] + other * turns[1], visit, 0)
    out_ref[...] = acc[...].astype(jnp.bfloat16)


def greet(targets):
    barrier = pltpu.get_barrier_semaphore()
    for target in targets:
        pl.semaphore_signal(barrier, inc=1, device_id=target, device_id_type=MESH_ID)
    pl.semaphore_wait(barrier, len(targets))


def row_peers(n_row, side=0):
    row, col, core, chip = place_of()
    if side:
        col = chip * CORES + 1 - core
    return [(lax.rem(row + d, n_row), col) for d in range(1, n_row)]


def sibling_peers(n_col):
    row, col, _, _ = place_of()
    return [(row, lax.rem(col + CORES * d, n_col)) for d in range(1, n_col // CORES)]


def partner_of():
    row, col, core, chip = place_of()
    return (row, chip * CORES + 1 - core)


def remote(src, dst, send_sem, recv_sem, target):
    return pltpu.make_async_remote_copy(
        src_ref=src,
        dst_ref=dst,
        send_sem=send_sem,
        recv_sem=recv_sem,
        device_id=target,
        device_id_type=MESH_ID,
    )


def send(*args):
    copy = remote(*args)
    copy.start()
    return copy


def prep_kernel(features_ref, out_ref):
    for tile in range(out_ref.shape[0]):
        block = features_ref[tile * TILE : (tile + 1) * TILE, :].astype(jnp.float32).T
        out_ref[tile] = block.astype(jnp.bfloat16)


def start_kernel(n_row, n_col, deg_a_ref, deg_b_ref, *refs):
    blocks = refs[:n_row]
    gathered_ref, root_ref, part, taken, theirs, roots = refs[n_row : n_row + 6]
    deg_send, deg_recv, near_send, near_recv, root_send, root_recv = refs[n_row + 6 :]
    row, col, core, chip = place_of()
    n_chip = n_col // CORES
    own = root_ref.shape[0]
    partner = partner_of()
    siblings = sibling_peers(n_col)
    mine, cross = row_peers(n_row), row_peers(n_row, 1)
    greet(siblings + mine + cross + [partner])
    part[...] = deg_a_ref[...] + deg_b_ref[...]
    copies = []
    for d, target in enumerate(siblings):
        start = (target[1] // CORES) * own
        copies.append(
            send(
                part.at[pl.ds(pl.multiple_of(start, own), own)],
                taken.at[d],
                deg_send.at[d],
                deg_recv.at[d],
                target,
            )
        )
    near = []
    for d in range(n_row):
        near.append(send(blocks[d], theirs.at[d], near_send.at[d], near_recv.at[d], partner))
    degree = part[pl.ds(pl.multiple_of(chip * own, own), own), :]
    for d, copy in enumerate(copies):
        copy.wait_recv()
        degree = degree + taken[d]
    root = lax.rsqrt(1.0 + degree)
    root_ref[...] = root
    roots[0, 0] = root
    root_copies = []
    for side, targets in ((0, mine), (1, [partner] + cross)):
        for d, target in enumerate(targets):
            d += 1 - side
            root_copies.append(
                send(roots.at[0, 0], roots.at[side, d], root_send.at[side, d], root_recv.at[side, d], target)
            )

    def scale(side, d, source, root):
        start = side * n_row * own + lax.rem(row + n_row - d, n_row) * own
        for tile in range(own):
            gathered_ref[start + tile] = (
                source[tile].astype(jnp.float32) * root[tile : tile + 1, :]
            ).astype(jnp.bfloat16)

    scale(0, 0, blocks[0], root)
    for copy in root_copies:
        copy.wait_recv()
    for d in range(1, n_row):
        scale(0, d, blocks[d], roots[0, d])
    for d in range(n_row):
        near[d].wait_recv()
        scale(1, d, theirs.at[d], roots[1, d])
    for copy in copies + near + root_copies:
        copy.wait_send()


def sum_kernel(n_row, n_col, spread, part_ref, root_ref, *refs):
    if spread:
        hop_ref, gathered_ref, comes, goes, *sems = refs
        send_sem, recv_sem, row_send, row_recv, near_send, near_recv = sems
    else:
        hop_ref, comes, goes, send_sem, recv_sem = refs
    row, col, core, chip = place_of()
    n_chip = n_col // CORES
    own = root_ref.shape[0]
    size = own // PIECES
    partner = partner_of()
    up = (row, lax.rem(col + CORES, n_col))
    down = (row, lax.rem(col + n_col - CORES, n_col))
    mine = row_peers(n_row)
    greet([up, down] + ([partner] + mine if spread else []))
    last = n_chip - 1

    low_half = chip < n_chip // 2
    early = jnp.where(low_half, 0, 1)

    def hop_copy(way, k, piece, direct):
        target = jnp.where(way == 0, last - k, k)
        start = pl.multiple_of(target * own, own) + piece * size
        source = part_ref.at[pl.ds(start, size)] if direct else goes.at[way, k, piece]
        return remote(
            source,
            comes.at[way, k, piece],
            send_sem.at[way, k, piece],
            recv_sem.at[way, k, piece],
            (row, lax.rem(col + jnp.where(way == 0, CORES, n_col - CORES), n_col)),
        )

    flow = [(k, piece) for k in range(last) for piece in range(PIECES)]
    timed = [(i, 0, *f) for i, f in enumerate(flow)]
    timed += [(i + RELAY_LAG, 1, *f) for i, f in enumerate(flow)]

    def steps():
        for _, late, k, piece in sorted(timed):
            way = 1 - early if late else early
            target = jnp.where(way == 0, last - k, k)
            ahead = jnp.where(way == 0, target - chip, chip - target) > 0
            first = chip == jnp.where(way == 0, 0, last)
            yield k, piece, way, target, ahead, first

    for k, piece, way, target, ahead, first in steps():

        @pl.when(ahead & first)
        def _():
            hop_copy(way, k, piece, True).start()

        @pl.when(ahead & jnp.logical_not(first))
        def _():
            hop_copy(way, k, piece, False).wait_recv()
            start = pl.multiple_of(target * own, own) + piece * size
            goes[way, k, piece] = (
                part_ref[pl.ds(start, size)].astype(jnp.float32)
                + comes[way, k, piece].astype(jnp.float32)
            ).astype(jnp.bfloat16)
            hop_copy(way, k, piece, False).start()

    row_copies, near_copies = {}, {}
    for piece in range(PIECES):
        for way, k, fed in ((0, last - chip, chip > 0), (1, chip, chip < last)):

            @pl.when(fed)
            def _():
                hop_copy(way, k, piece, False).wait_recv()

        total = part_ref[pl.ds(chip * own + piece * size, size)].astype(jnp.float32)
        below = comes[0, jnp.minimum(last - chip, last - 1), piece].astype(jnp.float32)
        above = comes[1, jnp.minimum(chip, last - 1), piece].astype(jnp.float32)
        total = total + jnp.where(chip > 0, below, 0.0) + jnp.where(chip < last, above, 0.0)
        roots = [root_ref[piece * size + tile : piece * size + tile + 1, :] for tile in range(size)]
        if spread:
            start = row * own + piece * size
            for tile in range(size):
                gathered_ref[start + tile] = (total[tile] * (roots[tile] * roots[tile])).astype(
                    jnp.bfloat16
                )
            for d, target in enumerate(mine):
                place = gathered_ref.at[pl.ds(start, size)]
                row_copies[piece, d] = send(
                    place, place, row_send.at[piece, d], row_recv.at[piece, d], target
                )
            near_copies[piece, 0] = send(
                gathered_ref.at[pl.ds(start, size)],
                gathered_ref.at[pl.ds(n_row * own + start, size)],
                near_send.at[piece, 0],
                near_recv.at[piece, 0],
                partner,
            )
        for tile in range(size):
            place = (piece * size + tile) * TILE
            hop_ref[place : place + TILE, :] = (total[tile] * roots[tile]).T.astype(jnp.bfloat16)
    for (piece, d), copy in row_copies.items():
        copy.wait_recv()
        start = lax.rem(row + n_row - d - 1, n_row) * own + piece * size
        near_copies[piece, d + 1] = send(
            gathered_ref.at[pl.ds(start, size)],
            gathered_ref.at[pl.ds(n_row * own + start, size)],
            near_send.at[piece, d + 1],
            near_recv.at[piece, d + 1],
            partner,
        )
    for copy in near_copies.values():
        copy.wait_recv()
    for copy in list(row_copies.values()) + list(near_copies.values()):
        copy.wait_send()
    for k, piece, way, target, ahead, first in steps():

        @pl.when(ahead)
        def _():
            hop_copy(way, k, piece, False).wait_send()


def sems(*shape):
    return pltpu.SemaphoreType.DMA(shape)


def comm_params(ident):
    return pltpu.CompilerParams(
        collective_id=ident, has_side_effects=True, vmem_limit_bytes=48 * 2**20
    )


def plain_params():
    return pltpu.CompilerParams(vmem_limit_bytes=48 * 2**20)


def local(features, tile_rows, tile_cols, edge_lists, tile_counts):
    node_count, feat_width = features.shape
    n_row, n_col = lax.axis_size("row"), lax.axis_size("col")
    n_chip = n_col // CORES
    own = node_count // TILE
    half_tiles = own * n_chip
    source_tiles = own * n_row
    slots = tile_rows.shape[-1]
    bf16, f32 = jnp.bfloat16, jnp.float32
    places = -(-(slots + CORES * half_tiles) // TILE) * TILE
    swap = [(i, i + 1 - 2 * (i % CORES)) for i in range(n_col)]

    edges_b = lax.ppermute(edge_lists, "col", swap)
    own_type = jax.ShapeDtypeStruct((own, feat_width, TILE), bf16)
    turned = pl.pallas_call(
        prep_kernel,
        out_shape=own_type,
        in_specs=[VMEM_SPEC],
        out_specs=VMEM_SPEC,
        name="prep",
    )(features)
    blocks = [turned] + [
        lax.ppermute(turned, "row", [(i, (i + d) % n_row) for i in range(n_row)])
        for d in range(1, n_row)
    ]

    order = pl.pallas_call(
        functools.partial(order_kernel, own, n_chip),
        out_shape=jax.ShapeDtypeStruct((8, places), jnp.int32),
        in_specs=[SMEM_SPEC, VMEM_SPEC, VMEM_SPEC],
        out_specs=VMEM_SPEC,
        compiler_params=plain_params(),
        name="order",
    )(tile_counts[0], tile_rows[0], tile_cols[0])
    order_b = lax.ppermute(order, "col", swap)

    def build(order, edges, other):
        edges = edges.reshape(2, slots, TILE)
        return pl.pallas_call(
            functools.partial(build_kernel, half_tiles, other),
            in_specs=[SMEM_SPEC]
            + [
                pl.BlockSpec((None, slots, TILE), lambda i, side=side: (side, 0, 0))
                for side in range(2)
            ],
            grid=(1,),
            out_specs=[ANY_SPEC, pl.BlockSpec((half_tiles, TILE), lambda i: (0, 0))],
            scratch_shapes=[
                pltpu.VMEM((2, BUILD_UNROLL // 2, 2 * TILE, TILE), bf16),
                pltpu.VMEM((half_tiles, 8, TILE), f32),
                sems(2),
            ],
            out_shape=[
                jax.ShapeDtypeStruct((places // 2, 2 * TILE, TILE), bf16),
                jax.ShapeDtypeStruct((half_tiles, TILE), f32),
            ],
            compiler_params=plain_params(),
            cost_estimate=pl.CostEstimate(flops=10**10, bytes_accessed=0, transcendentals=0),
            name="build",
        )(order, edges, edges)

    store_a, degree_a = build(order, edge_lists, False)
    store_b, degree_b = build(order_b, edges_b, True)

    gathered_type = jax.ShapeDtypeStruct((CORES * source_tiles, feat_width, TILE), bf16)
    gathered, root = pl.pallas_call(
        functools.partial(start_kernel, n_row, n_col),
        out_shape=[gathered_type, jax.ShapeDtypeStruct((own, TILE), f32)],
        in_specs=[VMEM_SPEC] * (2 + n_row),
        out_specs=[VMEM_SPEC] * 2,
        scratch_shapes=[
            pltpu.VMEM((half_tiles, TILE), f32),
            pltpu.VMEM((n_chip - 1, own, TILE), f32),
            pltpu.VMEM((n_row, own, feat_width, TILE), bf16),
            pltpu.VMEM((2, n_row, own, TILE), f32),
            sems(n_chip - 1),
            sems(n_chip - 1),
            sems(n_row),
            sems(n_row),
            sems(2, n_row),
            sems(2, n_row),
        ],
        compiler_params=comm_params(0),
        name="start",
    )(degree_a, degree_b, *blocks)

    def apply(sources):
        def body(order_a, order_b, store_a, store_b, *refs):
            apply_kernel(half_tiles, (order_a, order_b), (store_a, store_b), *refs)

        return pl.pallas_call(
            body,
            in_specs=[SMEM_SPEC] * 2 + [ANY_SPEC] * 2 + [VMEM_SPEC],
            out_specs=VMEM_SPEC,
            scratch_shapes=[
                pltpu.VMEM((APPLY_SLOTS, APPLY_UNROLL // 2, 2 * TILE, TILE), bf16),
                pltpu.VMEM((half_tiles, feat_width, TILE), f32),
                sems(APPLY_SLOTS),
            ],
            out_shape=jax.ShapeDtypeStruct((half_tiles, feat_width, TILE), bf16),
            compiler_params=plain_params(),
            name="apply",
        )(order, order_b, store_a, store_b, sources)

    def collect(part, spread):
        size = own // PIECES
        outs = [jax.ShapeDtypeStruct((node_count, feat_width), bf16)]
        semaphores = [sems(2, n_chip - 1, PIECES)] * 2
        if spread:
            outs.append(gathered_type)
            semaphores += [sems(PIECES, n_row - 1)] * 2 + [sems(PIECES, n_row)] * 2
        return pl.pallas_call(
            functools.partial(sum_kernel, n_row, n_col, spread),
            out_shape=outs,
            in_specs=[VMEM_SPEC] * 2,
            out_specs=[VMEM_SPEC] * len(outs),
            scratch_shapes=[pltpu.VMEM((2, n_chip - 1, PIECES, size, feat_width, TILE), bf16)] * 2
            + semaphores,
            compiler_params=comm_params(1 if spread else 2),
            name="spread" if spread else "finish",
        )(part, root)

    hop_one, gathered = collect(apply(gathered), True)
    (hop_two,) = collect(apply(gathered), False)
    return (hop_one, hop_two)


def solution(mesh):
    placed = (
        P(("row", "col"), None),
        P("row", "col", None),
        P("row", "col", None),
        P(None, "row", "col", None, None),
        P("row", "col"),
    )
    return jax.shard_map(
        local,
        mesh=mesh,
        in_specs=placed,
        out_specs=(P(("row", "col"), None), P(("row", "col"), None)),
        check_vma=False,
    )
```

```python
import functools

import jax
import jax.numpy as jnp
from jax import lax
from jax.experimental import pallas as pl
from jax.experimental.pallas import tpu as pltpu
from jax.sharding import PartitionSpec as P

TILE = 128
ROWS_MIN = 16
BUILD_UNROLL = 32
BUILD_SLOTS = 6
APPLY_UNROLL = 32
APPLY_SLOTS = 4
HOT = jnp.float8_e4m3fn
HOT_ROWS = 32
EXTRA = 16
PIECES = 4
RELAY_LAG = 3
EARLY = 1
CORES = 2
MESH_ID = pl.DeviceIdType.MESH
VMEM_SPEC = pl.BlockSpec(memory_space=pltpu.VMEM)
SMEM_SPEC = pl.BlockSpec(memory_space=pltpu.SMEM)
ANY_SPEC = pl.BlockSpec(memory_space=pl.ANY)


def place_of():
    row, col = lax.axis_index("row"), lax.axis_index("col")
    return row, col, lax.rem(col, CORES), col // CORES


def order_kernel(own, n_chip, count_ref, rows_ref, cols_ref, order_ref):
    slots = rows_ref.shape[-1]
    places = order_ref.shape[-1]
    bins = CORES * n_chip * own
    bf16, f32 = jnp.bfloat16, jnp.float32
    _, _, core, chip = place_of()

    def iota(shape, dim):
        return lax.broadcasted_iota(jnp.int32, shape, dim)

    def hot(mask):
        return jnp.where(mask, 1.0, 0.0).astype(bf16)

    def mul(x, y):
        return jnp.dot(x.astype(bf16), y.astype(bf16), preferred_element_type=f32)

    slot = iota((1, slots), 1)
    alive = slot < count_ref[0]
    rows = jnp.where(alive, rows_ref[...], 0)
    cols = jnp.where(alive, cols_ref[...], 0)
    owner = rows // own
    target = owner // CORES
    other = jnp.where(lax.rem(owner, CORES) == core, 0, 1)
    rank = jnp.where(chip < n_chip // 2, n_chip - 1 - target, target)
    within = lax.rem(rows, own)
    bin_of = jnp.where(alive, (other * n_chip + rank) * own + within, -1)
    local = rank * own + within
    belongs = bin_of == iota((bins, slots), 0)
    ranks = mul(hot(belongs), hot(iota((slots, slots), 0) <= iota((slots, slots), 1)))
    totals = jnp.broadcast_to(ranks[:, slots - 1 :], (bins, TILE)).astype(jnp.int32)
    pairs = (totals + 1) // 2
    before = hot(iota((bins, bins), 1) < iota((bins, bins), 0))
    offsets = 2.0 * (
        32.0 * mul(before, (pairs // 32).astype(f32)) + mul(before, (pairs % 32).astype(f32))
    )
    spots = jnp.where(belongs, ranks - 1.0 + offsets[:, :1], 0.0)
    spot = jnp.where(alive, jnp.sum(spots, axis=0, keepdims=True), -1.0)
    spot = jnp.broadcast_to(spot, (TILE, slots)).T.astype(jnp.int32)
    facts = [slot // 32, slot % 32, jnp.where(alive, 1, 0), local, cols]
    facts = jnp.concatenate(
        [fact.astype(f32) for fact in facts] + [jnp.zeros((EXTRA - len(facts), slots), f32)], axis=0
    )
    for block in range(places // TILE):
        taken = hot(spot == iota((slots, TILE), 1) + block * TILE)
        found = mul(facts, taken).astype(jnp.int32)
        place = 32 * found[0:1] + found[1:2] + found[2:3] - 1
        order_ref[:, block * TILE : (block + 1) * TILE] = jnp.concatenate(
            [place, found[3:5], jnp.zeros((5, TILE), jnp.int32)], axis=0
        )
    order_ref[3:4, 0:bins] = offsets.T[0:1, :].astype(jnp.int32)
    end = jnp.sum(2.0 * pairs.astype(f32), axis=0, keepdims=True).astype(jnp.int32)
    order_ref[4:5, 0:TILE] = end


def span_of(order_ref, half_bins, other):
    middle = order_ref[3, half_bins]
    if other:
        return middle, order_ref[4, 0]
    return 0, middle


def build_kernel(half_bins, other, order_ref, dst_ref, src_ref, store_ref, degree_ref, made, degree_acc, sem):
    degree_acc[...] = jnp.zeros_like(degree_acc)
    low, high = span_of(order_ref, half_bins, other)
    turns = (high - low + BUILD_UNROLL - 1) // BUILD_UNROLL
    pairs = BUILD_UNROLL // 2
    cells = [
        (lax.broadcasted_iota(jnp.int32, (HOT_ROWS, TILE), 0) + start).astype(jnp.int8)
        for start in range(0, TILE, HOT_ROWS)
    ]

    def hot(ids):
        ids = jnp.broadcast_to(ids, (HOT_ROWS, TILE)).astype(jnp.int8)
        return jnp.concatenate(
            [jnp.where(ids == cell, HOT(1), HOT(0)) for cell in cells], axis=0
        )

    def out_copy(turn):
        side = lax.rem(turn, BUILD_SLOTS)
        return pltpu.make_async_copy(
            made.at[side], store_ref.at[pl.ds(turn * pairs, pairs)], sem.at[side]
        )

    def visit(turn, carry):
        side = lax.rem(turn, BUILD_SLOTS)

        @pl.when(turn >= BUILD_SLOTS)
        def _():
            out_copy(turn - BUILD_SLOTS).wait()

        for pair in range(pairs):
            counts = []
            base = low + turn * BUILD_UNROLL + 2 * pair
            for half in range(2):
                slot = jnp.where(base < high, order_ref[0, base + half], -1)
                safe = jnp.maximum(slot, 0)
                dst = jnp.where(slot >= 0, dst_ref[pl.ds(safe, 1), :], -1)
                src = src_ref[pl.ds(safe, 1), :]
                both = lax.dot_general(
                    hot(src), hot(dst), (((1,), (1,)), ((), ())), preferred_element_type=jnp.float32
                )
                made[side, pair, half * TILE : (half + 1) * TILE] = both.astype(jnp.bfloat16)
                counts.append(jnp.sum(both.reshape(TILE // 8, 8, TILE), axis=0))
            degree_acc[order_ref[1, base]] += counts[0] + counts[1]
        out_copy(turn).start()
        return carry

    lax.fori_loop(0, turns, visit, 0)

    for back in range(BUILD_SLOTS, 0, -1):

        @pl.when(turns >= back)
        def _():
            out_copy(turns - back).wait()

    degree_ref[...] = jnp.sum(degree_acc[...], axis=1)


def apply_kernel(half_bins, first_row, orders, stores, source_ref, out_ref, held, acc, sem):
    acc[...] = jnp.zeros_like(acc)
    rows = out_ref.shape[0]
    pairs = APPLY_UNROLL // 2
    lists = [span_of(order, half_bins, other)[0] for other, order in enumerate(orders)]
    spans = []
    for other, order in enumerate(orders):
        bins = (other * half_bins + first_row, other * half_bins + first_row + rows)
        end = order[4, 0] if bins[1] == 2 * half_bins else order[3, bins[1]]
        spans.append((order[3, bins[0]], end))
    turns = [(high - low + APPLY_UNROLL - 1) // APPLY_UNROLL for low, high in spans]

    def fetch(turn):
        slot = lax.rem(turn, APPLY_SLOTS)
        for other in range(2):
            local = turn - other * turns[0]

            @pl.when((local >= 0) & (local < turns[other]))
            def _():
                start = (spans[other][0] - lists[other]) // 2 + local * pairs
                pltpu.make_async_copy(
                    stores[other].at[pl.ds(start, pairs)], held.at[slot], sem.at[slot]
                ).start()

    for turn in range(APPLY_SLOTS - 1):
        fetch(turn)

    for other in range(2):
        order_ref = orders[other]
        low, high = spans[other]
        offset = other * source_ref.shape[0] // 2

        def visit(turn, carry):
            slot = lax.rem(turn, APPLY_SLOTS)
            pltpu.make_async_copy(
                stores[0].at[pl.ds(0, pairs)], held.at[slot], sem.at[slot]
            ).wait()
            fetch(turn + APPLY_SLOTS - 1)
            for pair in range(pairs):
                base = low + (turn - other * turns[0]) * APPLY_UNROLL + 2 * pair
                sources = jnp.concatenate(
                    [
                        source_ref[offset + order_ref[2, base]],
                        source_ref[offset + order_ref[2, base + 1]],
                    ],
                    axis=1,
                )
                place = jnp.where(base < high, order_ref[1, base] - first_row, rows)
                acc[place] += jnp.dot(
                    sources, held[slot, pair], preferred_element_type=jnp.float32
                )
            return carry

        lax.fori_loop(other * turns[0], turns[0] + other * turns[1], visit, 0)
    out_ref[...] = acc[:rows].astype(jnp.bfloat16)


def greet(targets):
    barrier = pltpu.get_barrier_semaphore()
    for target in targets:
        pl.semaphore_signal(barrier, inc=1, device_id=target, device_id_type=MESH_ID)
    pl.semaphore_wait(barrier, len(targets))


def row_peers(n_row, side=0):
    row, col, core, chip = place_of()
    if side:
        col = chip * CORES + 1 - core
    return [(lax.rem(row + d, n_row), col) for d in range(1, n_row)]


def sibling_peers(n_col):
    row, col, _, _ = place_of()
    return [(row, lax.rem(col + CORES * d, n_col)) for d in range(1, n_col // CORES)]


def partner_of():
    row, col, core, chip = place_of()
    return (row, chip * CORES + 1 - core)


def remote(src, dst, send_sem, recv_sem, target):
    return pltpu.make_async_remote_copy(
        src_ref=src,
        dst_ref=dst,
        send_sem=send_sem,
        recv_sem=recv_sem,
        device_id=target,
        device_id_type=MESH_ID,
    )


def send(*args):
    copy = remote(*args)
    copy.start()
    return copy


def prep_kernel(features_ref, out_ref):
    for tile in range(out_ref.shape[0]):
        block = features_ref[tile * TILE : (tile + 1) * TILE, :].astype(jnp.float32).T
        out_ref[tile] = block.astype(jnp.bfloat16)


def start_kernel(n_row, n_col, deg_a_ref, deg_b_ref, *refs):
    blocks = refs[:n_row]
    gathered_ref, root_ref, part, taken, theirs, roots = refs[n_row : n_row + 6]
    deg_send, deg_recv, near_send, near_recv, root_send, root_recv = refs[n_row + 6 :]
    row, col, core, chip = place_of()
    n_chip = n_col // CORES
    own = root_ref.shape[0]
    partner = partner_of()
    siblings = sibling_peers(n_col)
    mine, cross = row_peers(n_row), row_peers(n_row, 1)
    greet(siblings + mine + cross + [partner])
    part[...] = deg_a_ref[...] + deg_b_ref[...]
    copies = []
    low_half = chip < n_chip // 2
    for d, target in enumerate(siblings):
        rank = target[1] // CORES
        start = jnp.where(low_half, n_chip - 1 - rank, rank) * own
        copies.append(
            send(
                part.at[pl.ds(pl.multiple_of(start, own), own)],
                taken.at[d],
                deg_send.at[d],
                deg_recv.at[d],
                target,
            )
        )
    near = []
    for d in range(n_row):
        near.append(send(blocks[d], theirs.at[d], near_send.at[d], near_recv.at[d], partner))
    mine_rank = jnp.where(low_half, n_chip - 1 - chip, chip)
    degree = part[pl.ds(pl.multiple_of(mine_rank * own, own), own), :]
    for d, copy in enumerate(copies):
        copy.wait_recv()
        degree = degree + taken[d]
    root = lax.rsqrt(1.0 + degree)
    root_ref[...] = root
    roots[0, 0] = root
    root_copies = []
    for side, targets in ((0, mine), (1, [partner] + cross)):
        for d, target in enumerate(targets):
            d += 1 - side
            root_copies.append(
                send(roots.at[0, 0], roots.at[side, d], root_send.at[side, d], root_recv.at[side, d], target)
            )

    def scale(side, d, source, root):
        start = side * n_row * own + lax.rem(row + n_row - d, n_row) * own
        for tile in range(own):
            gathered_ref[start + tile] = (
                source[tile].astype(jnp.float32) * root[tile : tile + 1, :]
            ).astype(jnp.bfloat16)

    scale(0, 0, blocks[0], root)
    for copy in root_copies:
        copy.wait_recv()
    for d in range(1, n_row):
        scale(0, d, blocks[d], roots[0, d])
    for d in range(n_row):
        near[d].wait_recv()
        scale(1, d, theirs.at[d], roots[1, d])
    for copy in copies + near + root_copies:
        copy.wait_send()


def sum_kernel(n_row, n_col, spread, *refs):
    parts, given, refs = refs[: EARLY + 1], refs[EARLY + 1 : 2 * EARLY + 1], refs[2 * EARLY + 1 :]
    if spread:
        root_ref, hop_ref, gathered_ref, comes, goes, *sems = refs
        send_sem, recv_sem, row_send, row_recv, near_send, near_recv = sems
    else:
        root_ref, hop_ref, comes, goes, send_sem, recv_sem = refs
    row, col, core, chip = place_of()
    n_chip = n_col // CORES
    own = root_ref.shape[0]
    size = own // PIECES
    partner = partner_of()
    up = (row, lax.rem(col + CORES, n_col))
    down = (row, lax.rem(col + n_col - CORES, n_col))
    mine = row_peers(n_row)
    greet([up, down] + ([partner] + mine if spread else []))
    last = n_chip - 1
    low_half = chip < n_chip // 2
    early = jnp.where(low_half, 0, 1)
    depth = jnp.where(low_half, chip, last - chip)

    def block(rank, piece):
        if rank < EARLY:
            return parts[rank].at[piece * size : (piece + 1) * size]
        start = (rank - EARLY) * own + piece * size
        return parts[EARLY].at[start : start + size]

    def hop_copy(way, k, piece, source=None):
        return remote(
            goes.at[way, k, piece] if source is None else source,
            comes.at[way, k, piece],
            send_sem.at[way, k, piece],
            recv_sem.at[way, k, piece],
            (row, lax.rem(col + jnp.where(way == 0, CORES, n_col - CORES), n_col)),
        )

    flow = [(k, piece) for k in range(last) for piece in range(PIECES)]
    timed = [(i, 0, *f) for i, f in enumerate(flow)]
    timed += [(i + RELAY_LAG, 1, *f) for i, f in enumerate(flow) if f[0] < n_chip // 2 - 1]

    def steps():
        for _, late, k, piece in sorted(timed):
            way = 1 - early if late else early
            ahead = k < (depth if late else last - depth)
            yield k, piece, late, way, ahead

    for k, piece, late, way, ahead in steps():
        source = block(last - k if late else k, piece)

        def relay(arrived):
            goes[way, k, piece] = (
                source[...].astype(jnp.float32) + arrived.astype(jnp.float32)
            ).astype(jnp.bfloat16)
            hop_copy(way, k, piece).start()

        def relay_waited():
            hop_copy(way, k, piece).wait_recv()
            relay(comes[way, k, piece])

        if late:
            pl.when(ahead)(relay_waited)
        elif k >= EARLY:
            pl.when(ahead & (depth == 0))(lambda: hop_copy(way, k, piece, source).start())
            pl.when(ahead & (depth > 0))(relay_waited)
        else:
            pl.when(ahead & (depth == 1))(
                lambda: relay(given[k][piece * size : (piece + 1) * size])
            )
            pl.when(ahead & (depth > 1))(relay_waited)

    row_copies, near_copies = {}, {}
    for piece in range(PIECES):
        early_k = jnp.minimum(last - depth, last - 1)

        @pl.when(depth > 0)
        def _():
            hop_copy(early, early_k, piece).wait_recv()

        hop_copy(1 - early, depth, piece).wait_recv()
        start = pl.multiple_of((last - depth - EARLY) * own, own) + piece * size
        total = parts[EARLY][pl.ds(start, size)].astype(jnp.float32)
        near = comes[early, early_k, piece].astype(jnp.float32)
        total = total + jnp.where(depth > 0, near, 0.0)
        total = total + comes[1 - early, depth, piece].astype(jnp.float32)
        roots = [root_ref[piece * size + tile : piece * size + tile + 1, :] for tile in range(size)]
        if spread:
            start = row * own + piece * size
            for tile in range(size):
                gathered_ref[start + tile] = (total[tile] * (roots[tile] * roots[tile])).astype(
                    jnp.bfloat16
                )
            for d, target in enumerate(mine):
                place = gathered_ref.at[pl.ds(start, size)]
                row_copies[piece, d] = send(
                    place, place, row_send.at[piece, d], row_recv.at[piece, d], target
                )
            near_copies[piece, 0] = send(
                gathered_ref.at[pl.ds(start, size)],
                gathered_ref.at[pl.ds(n_row * own + start, size)],
                near_send.at[piece, 0],
                near_recv.at[piece, 0],
                partner,
            )
        for tile in range(size):
            place = (piece * size + tile) * TILE
            hop_ref[place : place + TILE, :] = (total[tile] * roots[tile]).T.astype(jnp.bfloat16)
    for (piece, d), copy in row_copies.items():
        copy.wait_recv()
        start = lax.rem(row + n_row - d - 1, n_row) * own + piece * size
        near_copies[piece, d + 1] = send(
            gathered_ref.at[pl.ds(start, size)],
            gathered_ref.at[pl.ds(n_row * own + start, size)],
            near_send.at[piece, d + 1],
            near_recv.at[piece, d + 1],
            partner,
        )
    for copy in near_copies.values():
        copy.wait_recv()
    for copy in list(row_copies.values()) + list(near_copies.values()):
        copy.wait_send()
    for k, piece, late, way, ahead in steps():
        if not late and k < EARLY:
            ahead = ahead & (depth > 0)
        pl.when(ahead)(lambda: hop_copy(way, k, piece).wait_send())


def sems(*shape):
    return pltpu.SemaphoreType.DMA(shape)


def comm_params(ident):
    return pltpu.CompilerParams(
        collective_id=ident, has_side_effects=True, vmem_limit_bytes=48 * 2**20
    )


def plain_params():
    return pltpu.CompilerParams(vmem_limit_bytes=48 * 2**20)


def local(features, tile_rows, tile_cols, edge_lists, tile_counts):
    node_count, feat_width = features.shape
    n_row, n_col = lax.axis_size("row"), lax.axis_size("col")
    n_chip = n_col // CORES
    own = node_count // TILE
    half_tiles = own * n_chip
    source_tiles = own * n_row
    slots = tile_rows.shape[-1]
    bf16, f32 = jnp.bfloat16, jnp.float32
    places = -(-(slots + CORES * half_tiles + max(BUILD_UNROLL, APPLY_UNROLL)) // TILE) * TILE
    swap = [(i, i + 1 - 2 * (i % CORES)) for i in range(n_col)]

    edges_b = lax.ppermute(edge_lists, "col", swap)
    own_type = jax.ShapeDtypeStruct((own, feat_width, TILE), bf16)
    turned = pl.pallas_call(
        prep_kernel,
        out_shape=own_type,
        in_specs=[VMEM_SPEC],
        out_specs=VMEM_SPEC,
        name="prep",
    )(features)
    blocks = [turned] + [
        lax.ppermute(turned, "row", [(i, (i + d) % n_row) for i in range(n_row)])
        for d in range(1, n_row)
    ]

    order = pl.pallas_call(
        functools.partial(order_kernel, own, n_chip),
        out_shape=jax.ShapeDtypeStruct((8, places), jnp.int32),
        in_specs=[SMEM_SPEC, VMEM_SPEC, VMEM_SPEC],
        out_specs=VMEM_SPEC,
        compiler_params=plain_params(),
        name="order",
    )(tile_counts[0], tile_rows[0], tile_cols[0])
    order_b = lax.ppermute(order, "col", swap)

    def build(order, edges, other):
        edges = edges.reshape(2, slots, TILE)
        return pl.pallas_call(
            functools.partial(build_kernel, half_tiles, other),
            in_specs=[SMEM_SPEC]
            + [
                pl.BlockSpec((None, slots, TILE), lambda i, side=side: (side, 0, 0))
                for side in range(2)
            ],
            grid=(1,),
            out_specs=[ANY_SPEC, pl.BlockSpec((half_tiles, TILE), lambda i: (0, 0))],
            scratch_shapes=[
                pltpu.VMEM((BUILD_SLOTS, BUILD_UNROLL // 2, 2 * TILE, TILE), bf16),
                pltpu.VMEM((half_tiles, 8, TILE), f32),
                sems(BUILD_SLOTS),
            ],
            out_shape=[
                jax.ShapeDtypeStruct((places // 2, 2 * TILE, TILE), bf16),
                jax.ShapeDtypeStruct((half_tiles, TILE), f32),
            ],
            compiler_params=plain_params(),
            cost_estimate=pl.CostEstimate(flops=10**10, bytes_accessed=0, transcendentals=0),
            name="build",
        )(order, edges, edges)

    store_a, degree_a = build(order, edge_lists, False)
    store_b, degree_b = build(order_b, edges_b, True)

    gathered_type = jax.ShapeDtypeStruct((CORES * source_tiles, feat_width, TILE), bf16)
    gathered, root = pl.pallas_call(
        functools.partial(start_kernel, n_row, n_col),
        out_shape=[gathered_type, jax.ShapeDtypeStruct((own, TILE), f32)],
        in_specs=[VMEM_SPEC] * (2 + n_row),
        out_specs=[VMEM_SPEC] * 2,
        scratch_shapes=[
            pltpu.VMEM((half_tiles, TILE), f32),
            pltpu.VMEM((n_chip - 1, own, TILE), f32),
            pltpu.VMEM((n_row, own, feat_width, TILE), bf16),
            pltpu.VMEM((2, n_row, own, TILE), f32),
            sems(n_chip - 1),
            sems(n_chip - 1),
            sems(n_row),
            sems(n_row),
            sems(2, n_row),
            sems(2, n_row),
        ],
        compiler_params=comm_params(0),
        name="start",
    )(degree_a, degree_b, *blocks)

    def apply(sources, ranks, after):
        rows = len(ranks) * own

        def body(order_a, order_b, store_a, store_b, sources, after, *refs):
            apply_kernel(
                half_tiles, ranks[0] * own, (order_a, order_b), (store_a, store_b), sources, *refs
            )

        return pl.pallas_call(
            body,
            in_specs=[SMEM_SPEC] * 2 + [ANY_SPEC] * 2 + [VMEM_SPEC, ANY_SPEC],
            out_specs=VMEM_SPEC,
            scratch_shapes=[
                pltpu.VMEM((APPLY_SLOTS, APPLY_UNROLL // 2, 2 * TILE, TILE), bf16),
                pltpu.VMEM((rows + 1, feat_width, TILE), f32),
                sems(APPLY_SLOTS),
            ],
            out_shape=jax.ShapeDtypeStruct((rows, feat_width, TILE), bf16),
            compiler_params=plain_params(),
            cost_estimate=pl.CostEstimate(flops=10**10, bytes_accessed=0, transcendentals=0),
            name="apply",
        )(order, order_b, store_a, store_b, sources, after)

    ends = [
        (a * CORES + core, b * CORES + core)
        for a, b in ((0, 1), (n_chip - 1, n_chip - 2))
        for core in range(CORES)
    ]

    def apply_all(sources):
        parts, given, after = [], [], sources
        for rank in range(EARLY):
            parts.append(apply(sources, [rank], after))
            given.append(lax.ppermute(parts[-1], "col", ends))
            after = parts[-1]
        parts.append(apply(sources, list(range(EARLY, n_chip)), after))
        return parts + given

    def collect(parts, spread):
        size = own // PIECES
        outs = [jax.ShapeDtypeStruct((node_count, feat_width), bf16)]
        semaphores = [sems(2, n_chip - 1, PIECES)] * 2
        if spread:
            outs.append(gathered_type)
            semaphores += [sems(PIECES, n_row - 1)] * 2 + [sems(PIECES, n_row)] * 2
        return pl.pallas_call(
            functools.partial(sum_kernel, n_row, n_col, spread),
            out_shape=outs,
            in_specs=[VMEM_SPEC] * (len(parts) + 1),
            out_specs=[VMEM_SPEC] * len(outs),
            scratch_shapes=[pltpu.VMEM((2, n_chip - 1, PIECES, size, feat_width, TILE), bf16)] * 2
            + semaphores,
            compiler_params=comm_params(1 if spread else 2),
            name="spread" if spread else "finish",
        )(*parts, root)

    hop_one, gathered = collect(apply_all(gathered), True)
    (hop_two,) = collect(apply_all(gathered), False)
    return (hop_one, hop_two)


def solution(mesh):
    placed = (
        P(("row", "col"), None),
        P("row", "col", None),
        P("row", "col", None),
        P(None, "row", "col", None, None),
        P("row", "col"),
    )
    return jax.shard_map(
        local,
        mesh=mesh,
        in_specs=placed,
        out_specs=(P(("row", "col"), None), P(("row", "col"), None)),
        check_vma=False,
    )
```

```python
import functools

import jax
import jax.numpy as jnp
from jax import lax
from jax.experimental import pallas as pl
from jax.experimental.pallas import tpu as pltpu
from jax.sharding import PartitionSpec as P

TILE = 128
ROWS_MIN = 16
BUILD_UNROLL = 32
BUILD_SLOTS = 6
APPLY_UNROLL = 64
APPLY_SLOTS = 4
HOT = jnp.float8_e4m3fn
HOT_ROWS = 32
EXTRA = 16
SLOT_BITS = 11
CODE_BITS = 8
PIECES = 4
RELAY_LAG = 3
EARLY = 1
CORES = 2
MESH_ID = pl.DeviceIdType.MESH
VMEM_SPEC = pl.BlockSpec(memory_space=pltpu.VMEM)
SMEM_SPEC = pl.BlockSpec(memory_space=pltpu.SMEM)
ANY_SPEC = pl.BlockSpec(memory_space=pl.ANY)
HBM_SPEC = pl.BlockSpec(memory_space=pltpu.HBM)


def place_of():
    row, col = lax.axis_index("row"), lax.axis_index("col")
    return row, col, lax.rem(col, CORES), col // CORES


def order_kernel(
    own, n_chip, pairs, count_ref, rows_hbm, cols_hbm, features_hbm,
    order_ref, turned_ref, rows_ref, cols_ref, features_ref, sem
):
    loads = [
        pltpu.make_async_copy(source, target, sem.at[i])
        for i, (source, target) in enumerate(
            (
                (rows_hbm, rows_ref),
                (cols_hbm, cols_ref),
                (features_hbm, features_ref),
            )
        )
    ]
    for load in loads:
        load.start()
    slots = rows_ref.shape[-1]
    bins = CORES * n_chip * own
    bf16, f32 = jnp.bfloat16, jnp.float32
    _, _, core, chip = place_of()

    def iota(shape, dim):
        return lax.broadcasted_iota(jnp.int32, shape, dim)

    def hot(mask):
        return jnp.where(mask, 1.0, 0.0).astype(bf16)

    def mul(x, y):
        return jnp.dot(x.astype(bf16), y.astype(bf16), preferred_element_type=f32)

    loads[0].wait()
    loads[1].wait()
    slot = iota((1, slots), 1)
    alive = slot < count_ref[0]
    rows = jnp.where(alive, rows_ref[...], 0)
    cols = jnp.where(alive, cols_ref[...], 0)
    owner = rows // own
    target = owner // CORES
    other = jnp.where(lax.rem(owner, CORES) == core, 0, 1)
    rank = jnp.where(chip < n_chip // 2, n_chip - 1 - target, target)
    local = rank * own + lax.rem(rows, own)
    bin_of = jnp.where(alive, other * n_chip * own + local, -1)
    belongs = bin_of == iota((bins, slots), 0)
    ranks = mul(hot(belongs), hot(iota((slots, slots), 0) <= iota((slots, slots), 1)))
    totals = jnp.broadcast_to(ranks[:, slots - 1 :], (bins, TILE)).astype(jnp.int32)
    halves = (totals + 1) // 2
    before = hot(iota((bins, bins), 1) < iota((bins, bins), 0))
    offsets = 32.0 * mul(before, (halves // 32).astype(f32)) + mul(before, (halves % 32).astype(f32))
    spots = jnp.where(belongs, ranks - 1.0 + 2.0 * offsets[:, :1], 0.0)
    spot = jnp.where(alive, jnp.sum(spots, axis=0, keepdims=True), -1.0)
    odd = jnp.where(alive, spot.astype(jnp.int32) % 2, -1)
    facts = []
    for side in range(2):
        here = odd == side
        facts += [
            jnp.where(here, fact, 0)
            for fact in (slot // 32, slot % 32, jnp.where(here, 1, 0), cols, local)
        ]
    facts = jnp.concatenate(
        [fact.astype(f32) for fact in facts] + [jnp.zeros((EXTRA - len(facts), slots), f32)], axis=0
    )
    pair_of = jnp.broadcast_to(spot, (TILE, slots)).T.astype(jnp.int32) >> 1
    for start in range(0, pairs, TILE):
        found = mul(facts, hot(pair_of == iota((slots, TILE), 1) + start)).astype(jnp.int32)
        places = [32 * found[i : i + 1] + found[i + 1 : i + 2] + found[i + 2 : i + 3] for i in (0, 5)]
        row, cols = found[4:5], (found[3:4], found[8:9])
        order_ref[:, start : start + TILE] = (row << (2 * SLOT_BITS)) + (places[1] << SLOT_BITS) + places[0]
        order_ref[:, pairs + start : pairs + start + TILE] = (
            (cols[1] << (2 * CODE_BITS)) + (cols[0] << CODE_BITS) + row
        )
    end = jnp.sum(halves.astype(f32), axis=0, keepdims=True).astype(jnp.int32)
    order_ref[:, 2 * pairs : 2 * pairs + bins] = offsets.T[0:1, :].astype(jnp.int32)
    order_ref[:, 2 * pairs + bins : 2 * pairs + bins + TILE] = end
    loads[2].wait()
    for tile in range(own):
        block = features_ref[tile * TILE : (tile + 1) * TILE, :].astype(f32).T
        turned_ref[tile] = block.astype(bf16)


def spans_of(order_ref, pairs, half_bins, other, first, last):
    base = 2 * pairs + other * half_bins
    return order_ref[0, base], order_ref[0, base + first], order_ref[0, base + last]


def build_kernel(half_bins, other, order_ref, edges_ref, *refs):
    *previous, store_ref, degree_ref, made, degree_acc, sem = refs
    degree_acc[...] = jnp.zeros_like(degree_acc)
    _, low, high = spans_of(order_ref, store_ref.shape[0], half_bins, other, 0, half_bins)
    pairs = BUILD_UNROLL // 2
    turns = (high - low + pairs - 1) // pairs
    mask = 2**SLOT_BITS - 1
    cells = [
        (lax.broadcasted_iota(jnp.int32, (HOT_ROWS, TILE), 0) + start).astype(jnp.int8)
        for start in range(0, TILE, HOT_ROWS)
    ]

    def hot(ids):
        ids = jnp.broadcast_to(ids, (HOT_ROWS, TILE)).astype(jnp.int8)
        return jnp.concatenate(
            [jnp.where(ids == cell, HOT(1), HOT(0)) for cell in cells], axis=0
        )

    def out_copy(turn):
        side = lax.rem(turn, BUILD_SLOTS)
        return pltpu.make_async_copy(
            made.at[side], store_ref.at[pl.ds(turn * pairs, pairs)], sem.at[side]
        )

    def visit(turn, carry):
        side = lax.rem(turn, BUILD_SLOTS)

        @pl.when(turn >= BUILD_SLOTS)
        def _():
            out_copy(turn - BUILD_SLOTS).wait()

        for pair in range(pairs):
            counts = []
            base = low + turn * pairs + pair
            code = order_ref[0, base]
            live = jnp.where(base < high, code, 0)
            for half in range(2):
                slot = ((live >> (half * SLOT_BITS)) & mask) - 1
                safe = jnp.maximum(slot, 0)
                dst = jnp.where(slot >= 0, edges_ref[0, pl.ds(safe, 1), :], -1)
                src = edges_ref[1, pl.ds(safe, 1), :]
                both = lax.dot_general(
                    hot(src), hot(dst), (((1,), (1,)), ((), ())), preferred_element_type=jnp.float32
                )
                made[side, pair, half * TILE : (half + 1) * TILE] = both.astype(jnp.bfloat16)
                counts.append(jnp.sum(both.reshape(TILE // 8, 8, TILE), axis=0))
            degree_acc[live >> (2 * SLOT_BITS)] += counts[0] + counts[1]
        out_copy(turn).start()
        return carry

    lax.fori_loop(0, turns, visit, 0)

    for back in range(BUILD_SLOTS, 0, -1):

        @pl.when(turns >= back)
        def _():
            out_copy(turns - back).wait()

    degree = jnp.sum(degree_acc[...], axis=1)
    degree_ref[...] = degree + previous[0][...] if previous else degree


def apply_kernel(half_bins, first_row, orders, stores, source_ref, out_ref, held, acc, sem):
    rows = out_ref.shape[0]
    pairs = APPLY_UNROLL // 2
    total_pairs = stores[0].shape[0]
    lists, spans, turns = [], [], []
    for other, order_ref in enumerate(orders):
        start, low, high = spans_of(
            order_ref, total_pairs, half_bins, other, first_row, first_row + rows
        )
        lists.append(start)
        spans.append((low, high))
        turns.append((high - low + pairs - 1) // pairs)
    code_mask = 2**CODE_BITS - 1

    def fetch(turn):
        slot = lax.rem(turn, APPLY_SLOTS)
        for other in range(2):
            local = turn - other * turns[0]

            @pl.when((local >= 0) & (local < turns[other]))
            def _():
                start = spans[other][0] - lists[other] + local * pairs
                pltpu.make_async_copy(
                    stores[other].at[pl.ds(start, pairs)], held.at[slot], sem.at[slot]
                ).start()

    for turn in range(APPLY_SLOTS - 1):
        fetch(turn)
    acc[...] = jnp.zeros_like(acc)

    for other in range(2):
        order_ref = orders[other]
        low, high = spans[other]
        offset = other * source_ref.shape[0] // 2

        def visit(turn, carry):
            slot = lax.rem(turn, APPLY_SLOTS)
            pltpu.make_async_copy(
                stores[0].at[pl.ds(0, pairs)], held.at[slot], sem.at[slot]
            ).wait()
            fetch(turn + APPLY_SLOTS - 1)
            for pair in range(pairs):
                base = low + (turn - other * turns[0]) * pairs + pair
                code = order_ref[0, total_pairs + base]
                left = (code >> CODE_BITS) & code_mask
                right = code >> (2 * CODE_BITS)
                sources = jnp.concatenate(
                    [source_ref[offset + left], source_ref[offset + right]], axis=1
                )
                place = jnp.where(base < high, (code & code_mask) - first_row, rows)
                acc[place] += jnp.dot(
                    sources, held[slot, pair], preferred_element_type=jnp.float32
                )
            return carry

        lax.fori_loop(other * turns[0], turns[0] + other * turns[1], visit, 0)
    out_ref[...] = acc[:rows].astype(jnp.bfloat16)


def greet(targets):
    barrier = pltpu.get_barrier_semaphore()
    for target in targets:
        pl.semaphore_signal(barrier, inc=1, device_id=target, device_id_type=MESH_ID)
    pl.semaphore_wait(barrier, len(targets))


def row_peers(n_row, side=0):
    row, col, core, chip = place_of()
    if side:
        col = chip * CORES + 1 - core
    return [(lax.rem(row + d, n_row), col) for d in range(1, n_row)]


def sibling_peers(n_col):
    row, col, _, _ = place_of()
    return [(row, lax.rem(col + CORES * d, n_col)) for d in range(1, n_col // CORES)]


def partner_of():
    row, col, core, chip = place_of()
    return (row, chip * CORES + 1 - core)


def remote(src, dst, send_sem, recv_sem, target):
    return pltpu.make_async_remote_copy(
        src_ref=src,
        dst_ref=dst,
        send_sem=send_sem,
        recv_sem=recv_sem,
        device_id=target,
        device_id_type=MESH_ID,
    )


def send(*args):
    copy = remote(*args)
    copy.start()
    return copy


def start_kernel(n_row, n_col, part, *refs):
    blocks = refs[:n_row]
    gathered_ref, root_ref, taken, theirs, roots = refs[n_row : n_row + 5]
    deg_send, deg_recv, near_send, near_recv, root_send, root_recv = refs[n_row + 5 :]
    row, col, core, chip = place_of()
    n_chip = n_col // CORES
    own = root_ref.shape[0]
    partner = partner_of()
    siblings = sibling_peers(n_col)
    mine, cross = row_peers(n_row), row_peers(n_row, 1)
    greet(siblings + mine + cross + [partner])
    copies = []
    low_half = chip < n_chip // 2
    for d, target in enumerate(siblings):
        rank = target[1] // CORES
        start = jnp.where(low_half, n_chip - 1 - rank, rank) * own
        copies.append(
            send(
                part.at[pl.ds(pl.multiple_of(start, own), own)],
                taken.at[d],
                deg_send.at[d],
                deg_recv.at[d],
                target,
            )
        )
    near = []
    for d in range(n_row):
        near.append(send(blocks[d], theirs.at[d], near_send.at[d], near_recv.at[d], partner))
    mine_rank = jnp.where(low_half, n_chip - 1 - chip, chip)
    degree = part[pl.ds(pl.multiple_of(mine_rank * own, own), own), :]
    for d, copy in enumerate(copies):
        copy.wait_recv()
        degree = degree + taken[d]
    root = lax.rsqrt(1.0 + degree)
    root_ref[...] = root
    roots[0, 0] = root
    root_copies = []
    for side, targets in ((0, mine), (1, [partner] + cross)):
        for d, target in enumerate(targets):
            d += 1 - side
            root_copies.append(
                send(roots.at[0, 0], roots.at[side, d], root_send.at[side, d], root_recv.at[side, d], target)
            )

    def scale(side, d, source, root):
        start = side * n_row * own + lax.rem(row + n_row - d, n_row) * own
        for tile in range(own):
            gathered_ref[start + tile] = (
                source[tile].astype(jnp.float32) * root[tile : tile + 1, :]
            ).astype(jnp.bfloat16)

    scale(0, 0, blocks[0], root)
    for copy in root_copies:
        copy.wait_recv()
    for d in range(1, n_row):
        scale(0, d, blocks[d], roots[0, d])
    for d in range(n_row):
        near[d].wait_recv()
        scale(1, d, theirs.at[d], roots[1, d])
    for copy in copies + near + root_copies:
        copy.wait_send()


def sum_kernel(n_row, n_col, spread, *refs):
    parts, given, refs = refs[: EARLY + 1], refs[EARLY + 1 : 2 * EARLY + 1], refs[2 * EARLY + 1 :]
    if spread:
        root_ref, hop_ref, gathered_ref, comes, goes, *sems = refs
        send_sem, recv_sem, row_send, row_recv, near_send, near_recv = sems
    else:
        root_ref, hop_ref, comes, goes, send_sem, recv_sem = refs
    row, col, core, chip = place_of()
    n_chip = n_col // CORES
    own = root_ref.shape[0]
    size = own // PIECES
    partner = partner_of()
    up = (row, lax.rem(col + CORES, n_col))
    down = (row, lax.rem(col + n_col - CORES, n_col))
    mine = row_peers(n_row)
    greet([up, down] + ([partner] + mine if spread else []))
    last = n_chip - 1
    low_half = chip < n_chip // 2
    early = jnp.where(low_half, 0, 1)
    depth = jnp.where(low_half, chip, last - chip)

    def block(rank, piece):
        if rank < EARLY:
            return parts[rank].at[piece * size : (piece + 1) * size]
        start = (rank - EARLY) * own + piece * size
        return parts[EARLY].at[start : start + size]

    def hop_copy(way, k, piece, source=None):
        return remote(
            goes.at[way, k, piece] if source is None else source,
            comes.at[way, k, piece],
            send_sem.at[way, k, piece],
            recv_sem.at[way, k, piece],
            (row, lax.rem(col + jnp.where(way == 0, CORES, n_col - CORES), n_col)),
        )

    flow = [(k, piece) for piece in range(PIECES) for k in range(last)]
    timed = [(i, 0, *f) for i, f in enumerate(flow)]
    timed += [(i + RELAY_LAG, 1, *f) for i, f in enumerate(flow) if f[0] < n_chip // 2 - 1]

    def steps():
        for _, late, k, piece in sorted(timed):
            way = 1 - early if late else early
            ahead = k < (depth if late else last - depth)
            yield k, piece, late, way, ahead

    for k, piece, late, way, ahead in steps():
        source = block(last - k if late else k, piece)

        def relay(arrived):
            goes[way, k, piece] = (
                source[...].astype(jnp.float32) + arrived.astype(jnp.float32)
            ).astype(jnp.bfloat16)
            hop_copy(way, k, piece).start()

        def relay_waited():
            hop_copy(way, k, piece).wait_recv()
            relay(comes[way, k, piece])

        if late:
            pl.when(ahead)(relay_waited)
        elif k >= EARLY:
            pl.when(ahead & (depth == 0))(lambda: hop_copy(way, k, piece, source).start())
            pl.when(ahead & (depth > 0))(relay_waited)
        else:
            pl.when(ahead & (depth == 1))(
                lambda: relay(given[k][piece * size : (piece + 1) * size])
            )
            pl.when(ahead & (depth > 1))(relay_waited)

    row_copies, near_copies = {}, {}
    for piece in range(PIECES):
        early_k = jnp.minimum(last - depth, last - 1)

        @pl.when(depth > 0)
        def _():
            hop_copy(early, early_k, piece).wait_recv()

        hop_copy(1 - early, depth, piece).wait_recv()
        start = pl.multiple_of((last - depth - EARLY) * own, own) + piece * size
        total = parts[EARLY][pl.ds(start, size)].astype(jnp.float32)
        near = comes[early, early_k, piece].astype(jnp.float32)
        total = total + jnp.where(depth > 0, near, 0.0)
        total = total + comes[1 - early, depth, piece].astype(jnp.float32)
        roots = [root_ref[piece * size + tile : piece * size + tile + 1, :] for tile in range(size)]
        if spread:
            start = row * own + piece * size
            for tile in range(size):
                gathered_ref[start + tile] = (total[tile] * (roots[tile] * roots[tile])).astype(
                    jnp.bfloat16
                )
            for d, target in enumerate(mine):
                place = gathered_ref.at[pl.ds(start, size)]
                row_copies[piece, d] = send(
                    place, place, row_send.at[piece, d], row_recv.at[piece, d], target
                )
            near_copies[piece, 0] = send(
                gathered_ref.at[pl.ds(start, size)],
                gathered_ref.at[pl.ds(n_row * own + start, size)],
                near_send.at[piece, 0],
                near_recv.at[piece, 0],
                partner,
            )
        for tile in range(size):
            place = (piece * size + tile) * TILE
            hop_ref[place : place + TILE, :] = (total[tile] * roots[tile]).T.astype(jnp.bfloat16)
    for (piece, d), copy in row_copies.items():
        copy.wait_recv()
        start = lax.rem(row + n_row - d - 1, n_row) * own + piece * size
        near_copies[piece, d + 1] = send(
            gathered_ref.at[pl.ds(start, size)],
            gathered_ref.at[pl.ds(n_row * own + start, size)],
            near_send.at[piece, d + 1],
            near_recv.at[piece, d + 1],
            partner,
        )
    for copy in near_copies.values():
        copy.wait_recv()
    for copy in list(row_copies.values()) + list(near_copies.values()):
        copy.wait_send()
    for k, piece, late, way, ahead in steps():
        if not late and k < EARLY:
            ahead = ahead & (depth > 0)
        pl.when(ahead)(lambda: hop_copy(way, k, piece).wait_send())


def sems(*shape):
    return pltpu.SemaphoreType.DMA(shape)


def comm_params(ident):
    return pltpu.CompilerParams(
        collective_id=ident, has_side_effects=True, vmem_limit_bytes=48 * 2**20
    )


def full_params():
    return pltpu.CompilerParams(vmem_limit_bytes=67043328)


def build_params():
    return pltpu.CompilerParams(vmem_limit_bytes=65 * 10**6)


def plain_params():
    return pltpu.CompilerParams(vmem_limit_bytes=48 * 2**20)


def local(features, tile_rows, tile_cols, edge_lists, tile_counts):
    node_count, feat_width = features.shape
    n_row, n_col = lax.axis_size("row"), lax.axis_size("col")
    n_chip = n_col // CORES
    own = node_count // TILE
    half_tiles = own * n_chip
    source_tiles = own * n_row
    slots = tile_rows.shape[-1]
    bf16, f32 = jnp.bfloat16, jnp.float32
    spare = max(BUILD_UNROLL, APPLY_UNROLL)
    pairs = -(-(slots + CORES * half_tiles + spare) // (2 * TILE)) * TILE
    swap = [(i, i + 1 - 2 * (i % CORES)) for i in range(n_col)]
    edges = edge_lists.reshape(2, slots, TILE)

    edges_b = lax.ppermute(edges, "col", swap)
    codes = 2 * pairs + -(-(CORES * half_tiles) // TILE) * TILE + TILE
    order, turned = pl.pallas_call(
        functools.partial(order_kernel, own, n_chip, pairs),
        out_shape=[
            jax.ShapeDtypeStruct((1, codes), jnp.int32),
            jax.ShapeDtypeStruct((own, feat_width, TILE), bf16),
        ],
        in_specs=[SMEM_SPEC] + [HBM_SPEC] * 3,
        out_specs=[VMEM_SPEC] * 2,
        scratch_shapes=[
            pltpu.VMEM((1, slots), jnp.int32),
            pltpu.VMEM((1, slots), jnp.int32),
            pltpu.VMEM((node_count, feat_width), bf16),
            sems(3),
        ],
        compiler_params=full_params(),
        name="order",
    )(tile_counts[0], tile_rows[0], tile_cols[0], features)
    blocks = [turned] + [
        lax.ppermute(turned, "row", [(i, (i + d) % n_row) for i in range(n_row)])
        for d in range(1, n_row)
    ]
    order_b = lax.ppermute(order, "col", swap)

    def build(order, edges, *previous):
        return pl.pallas_call(
            functools.partial(build_kernel, half_tiles, len(previous)),
            in_specs=[SMEM_SPEC, VMEM_SPEC] + [VMEM_SPEC] * len(previous),
            out_specs=[ANY_SPEC, VMEM_SPEC],
            scratch_shapes=[
                pltpu.VMEM((BUILD_SLOTS, BUILD_UNROLL // 2, 2 * TILE, TILE), bf16),
                pltpu.VMEM((half_tiles, 8, TILE), f32),
                sems(BUILD_SLOTS),
            ],
            out_shape=[
                jax.ShapeDtypeStruct((pairs, 2 * TILE, TILE), bf16),
                jax.ShapeDtypeStruct((half_tiles, TILE), f32),
            ],
            compiler_params=build_params(),
            cost_estimate=pl.CostEstimate(flops=10**10, bytes_accessed=0, transcendentals=0),
            name="build",
        )(order, edges, *previous)

    store_a, degree_a = build(order, edges)
    store_b, degree = build(order_b, edges_b, degree_a)

    gathered_type = jax.ShapeDtypeStruct((CORES * source_tiles, feat_width, TILE), bf16)
    gathered, root = pl.pallas_call(
        functools.partial(start_kernel, n_row, n_col),
        out_shape=[gathered_type, jax.ShapeDtypeStruct((own, TILE), f32)],
        in_specs=[VMEM_SPEC] * (1 + n_row),
        out_specs=[VMEM_SPEC] * 2,
        scratch_shapes=[
            pltpu.VMEM((n_chip - 1, own, TILE), f32),
            pltpu.VMEM((n_row, own, feat_width, TILE), bf16),
            pltpu.VMEM((2, n_row, own, TILE), f32),
            sems(n_chip - 1),
            sems(n_chip - 1),
            sems(n_row),
            sems(n_row),
            sems(2, n_row),
            sems(2, n_row),
        ],
        compiler_params=comm_params(0),
        name="start",
    )(degree, *blocks)

    def apply(sources, ranks, after):
        rows = len(ranks) * own

        def body(order_a, order_b, store_a, store_b, sources, after, *refs):
            apply_kernel(
                half_tiles, ranks[0] * own, (order_a, order_b), (store_a, store_b), sources, *refs
            )

        return pl.pallas_call(
            body,
            in_specs=[SMEM_SPEC] * 2 + [ANY_SPEC] * 2 + [VMEM_SPEC, ANY_SPEC],
            out_specs=VMEM_SPEC,
            scratch_shapes=[
                pltpu.VMEM((APPLY_SLOTS, APPLY_UNROLL // 2, 2 * TILE, TILE), bf16),
                pltpu.VMEM((rows + 1, feat_width, TILE), f32),
                sems(APPLY_SLOTS),
            ],
            out_shape=jax.ShapeDtypeStruct((rows, feat_width, TILE), bf16),
            compiler_params=plain_params(),
            cost_estimate=pl.CostEstimate(flops=10**10, bytes_accessed=0, transcendentals=0),
            name="apply",
        )(order, order_b, store_a, store_b, sources, after)

    ends = [
        (a * CORES + core, b * CORES + core)
        for a, b in ((0, 1), (n_chip - 1, n_chip - 2))
        for core in range(CORES)
    ]

    def apply_all(sources):
        parts, given, after = [], [], sources
        for rank in range(EARLY):
            parts.append(apply(sources, [rank], after))
            given.append(lax.ppermute(parts[-1], "col", ends))
            after = parts[-1]
        parts.append(apply(sources, list(range(EARLY, n_chip)), after))
        return parts + given

    def collect(parts, spread):
        size = own // PIECES
        outs = [jax.ShapeDtypeStruct((node_count, feat_width), bf16)]
        semaphores = [sems(2, n_chip - 1, PIECES)] * 2
        if spread:
            outs.append(gathered_type)
            semaphores += [sems(PIECES, n_row - 1)] * 2 + [sems(PIECES, n_row)] * 2
        return pl.pallas_call(
            functools.partial(sum_kernel, n_row, n_col, spread),
            out_shape=outs,
            in_specs=[VMEM_SPEC] * (len(parts) + 1),
            out_specs=[VMEM_SPEC] * len(outs),
            scratch_shapes=[pltpu.VMEM((2, n_chip - 1, PIECES, size, feat_width, TILE), bf16)] * 2
            + semaphores,
            compiler_params=comm_params(1 if spread else 2),
            name="spread" if spread else "finish",
        )(*parts, root)

    hop_one, gathered = collect(apply_all(gathered), True)
    (hop_two,) = collect(apply_all(gathered), False)
    return (hop_one, hop_two)


def solution(mesh):
    placed = (
        P(("row", "col"), None),
        P("row", "col", None),
        P("row", "col", None),
        P(None, "row", "col", None, None),
        P("row", "col"),
    )
    return jax.shard_map(
        local,
        mesh=mesh,
        in_specs=placed,
        out_specs=(P(("row", "col"), None), P(("row", "col"), None)),
        check_vma=False,
    )
```

```python
import functools

import jax
import jax.numpy as jnp
from jax import lax
from jax.experimental import pallas as pl
from jax.experimental.pallas import tpu as pltpu
from jax.sharding import PartitionSpec as P

TILE = 128
ROWS_MIN = 16
BUILD_UNROLL = 32
BUILD_SLOTS = 1
KEPT_PAIRS = 416
LATE_PAIRS = 8
APPLY_UNROLL = 64
APPLY_SLOTS = 4
HOT = jnp.float8_e4m3fn
HOT_ROWS = 32
EXTRA = 16
SLOT_BITS = 11
CODE_BITS = 8
PIECES = 4
RELAY_LAG = 3
EARLY = 1
CORES = 2
MESH_ID = pl.DeviceIdType.MESH
VMEM_SPEC = pl.BlockSpec(memory_space=pltpu.VMEM)
SMEM_SPEC = pl.BlockSpec(memory_space=pltpu.SMEM)
ANY_SPEC = pl.BlockSpec(memory_space=pl.ANY)
HBM_SPEC = pl.BlockSpec(memory_space=pltpu.HBM)


def place_of():
    row, col = lax.axis_index("row"), lax.axis_index("col")
    return row, col, lax.rem(col, CORES), col // CORES


def order_kernel(
    own, n_chip, pairs, count_ref, rows_hbm, cols_hbm, features_hbm,
    order_ref, turned_ref, rows_ref, cols_ref, features_ref, sem
):
    loads = [
        pltpu.make_async_copy(source, target, sem.at[i])
        for i, (source, target) in enumerate(
            (
                (rows_hbm, rows_ref),
                (cols_hbm, cols_ref),
                (features_hbm, features_ref),
            )
        )
    ]
    for load in loads:
        load.start()
    slots = rows_ref.shape[-1]
    bins = CORES * n_chip * own
    bf16, f32 = jnp.bfloat16, jnp.float32
    _, _, core, chip = place_of()

    def iota(shape, dim):
        return lax.broadcasted_iota(jnp.int32, shape, dim)

    def hot(mask):
        return jnp.where(mask, 1.0, 0.0).astype(bf16)

    def mul(x, y):
        return jnp.dot(x.astype(bf16), y.astype(bf16), preferred_element_type=f32)

    loads[0].wait()
    loads[1].wait()
    slot = iota((1, slots), 1)
    alive = slot < count_ref[0]
    rows = jnp.where(alive, rows_ref[...], 0)
    cols = jnp.where(alive, cols_ref[...], 0)
    owner = rows // own
    target = owner // CORES
    other = jnp.where(lax.rem(owner, CORES) == core, 0, 1)
    rank = jnp.where(chip < n_chip // 2, n_chip - 1 - target, target)
    local = rank * own + lax.rem(rows, own)
    bin_of = jnp.where(alive, other * n_chip * own + local, -1)
    belongs = bin_of == iota((bins, slots), 0)
    ranks = mul(hot(belongs), hot(iota((slots, slots), 0) <= iota((slots, slots), 1)))
    totals = jnp.broadcast_to(ranks[:, slots - 1 :], (bins, TILE)).astype(jnp.int32)
    halves = (totals + 1) // 2
    before = hot(iota((bins, bins), 1) < iota((bins, bins), 0))
    offsets = 32.0 * mul(before, (halves // 32).astype(f32)) + mul(before, (halves % 32).astype(f32))
    spots = jnp.where(belongs, ranks - 1.0 + 2.0 * offsets[:, :1], 0.0)
    spot = jnp.where(alive, jnp.sum(spots, axis=0, keepdims=True), -1.0)
    odd = jnp.where(alive, spot.astype(jnp.int32) % 2, -1)
    facts = []
    for side in range(2):
        here = odd == side
        facts += [
            jnp.where(here, fact, 0)
            for fact in (slot // 32, slot % 32, jnp.where(here, 1, 0), cols, local)
        ]
    facts = jnp.concatenate(
        [fact.astype(f32) for fact in facts] + [jnp.zeros((EXTRA - len(facts), slots), f32)], axis=0
    )
    pair_of = jnp.broadcast_to(spot, (TILE, slots)).T.astype(jnp.int32) >> 1
    for start in range(0, pairs, TILE):
        found = mul(facts, hot(pair_of == iota((slots, TILE), 1) + start)).astype(jnp.int32)
        places = [32 * found[i : i + 1] + found[i + 1 : i + 2] + found[i + 2 : i + 3] for i in (0, 5)]
        row, cols = found[4:5], (found[3:4], found[8:9])
        order_ref[:, start : start + TILE] = (row << (2 * SLOT_BITS)) + (places[1] << SLOT_BITS) + places[0]
        order_ref[:, pairs + start : pairs + start + TILE] = (
            (cols[1] << (2 * CODE_BITS)) + (cols[0] << CODE_BITS) + row
        )
    end = jnp.sum(halves.astype(f32), axis=0, keepdims=True).astype(jnp.int32)
    order_ref[:, 2 * pairs : 2 * pairs + bins] = offsets.T[0:1, :].astype(jnp.int32)
    order_ref[:, 2 * pairs + bins : 2 * pairs + bins + TILE] = end
    loads[2].wait()
    for tile in range(own):
        block = features_ref[tile * TILE : (tile + 1) * TILE, :].astype(f32).T
        turned_ref[tile] = block.astype(bf16)


def spans_of(order_ref, pairs, half_bins, other, first, last):
    base = 2 * pairs + other * half_bins
    return order_ref[0, base], order_ref[0, base + first], order_ref[0, base + last]


def lists_of(orders, total_pairs, half_bins, first, last):
    pairs = BUILD_UNROLL // 2
    spans, start = [], 0
    for other, order_ref in enumerate(orders):
        low, begin, end = spans_of(order_ref, total_pairs, half_bins, other, first, last)
        spans.append((start - low, begin, end))
        high = spans_of(order_ref, total_pairs, half_bins, other, 0, half_bins)[2]
        start = start + (high - low + pairs - 1) // pairs * pairs
    return spans, start // pairs


def build_kernel(
    half_bins, total_pairs, order_a, order_b, edges_a, edges_b, kept_ref, store_ref, degree_ref,
    edges_ref, made, degree_acc, sem, edge_sem
):
    loads = [
        pltpu.make_async_copy(source, edges_ref.at[i], edge_sem.at[i])
        for i, source in enumerate((edges_a, edges_b))
    ]
    for load in loads:
        load.start()
    degree_acc[...] = jnp.zeros_like(degree_acc)
    pairs = BUILD_UNROLL // 2
    (span_a, span_b), turns = lists_of((order_a, order_b), total_pairs, half_bins, 0, half_bins)
    turns_a = (span_b[0] + span_b[1]) // pairs
    kept_turns = jnp.minimum(turns, KEPT_PAIRS // pairs)
    mask = 2**SLOT_BITS - 1
    cells = [
        (lax.broadcasted_iota(jnp.int32, (HOT_ROWS, TILE), 0) + start).astype(jnp.int8)
        for start in range(0, TILE, HOT_ROWS)
    ]

    def hot(ids):
        ids = jnp.broadcast_to(ids, (HOT_ROWS, TILE)).astype(jnp.int8)
        return jnp.concatenate(
            [jnp.where(ids == cell, HOT(1), HOT(0)) for cell in cells], axis=0
        )

    def fill(turn, target):
        mine = turn < turns_a
        other = jnp.where(mine, 0, 1)
        high = jnp.where(mine, span_a[2], span_b[2])
        low = turn * pairs - jnp.where(mine, 0, span_b[0])
        for pair in range(pairs):
            counts = []
            base = low + pair
            code = jnp.where(mine, order_a[0, base], order_b[0, base])
            live = jnp.where(base < high, code, 0)
            for half in range(2):
                slot = ((live >> (half * SLOT_BITS)) & mask) - 1
                safe = jnp.maximum(slot, 0)
                dst = jnp.where(slot >= 0, edges_ref[other, 0, pl.ds(safe, 1), :], -1)
                src = edges_ref[other, 1, pl.ds(safe, 1), :]
                both = lax.dot_general(
                    hot(src), hot(dst), (((1,), (1,)), ((), ())), preferred_element_type=jnp.float32
                )
                target[pair, half * TILE : (half + 1) * TILE] = both.astype(jnp.bfloat16)
                counts.append(jnp.sum(both.reshape(TILE // 8, 8, TILE), axis=0))
            degree_acc[live >> (2 * SLOT_BITS)] += counts[0] + counts[1]

    def keep(turn, carry):
        fill(turn, kept_ref.at[pl.ds(turn * pairs, pairs)])
        return carry

    for load in loads:
        load.wait()
    lax.fori_loop(0, kept_turns, keep, 0)

    def out_copy(turn):
        side = lax.rem(turn, BUILD_SLOTS)
        return pltpu.make_async_copy(
            made.at[side], store_ref.at[pl.ds(turn * pairs, pairs)], sem.at[side]
        )

    def spill(turn, carry):
        @pl.when(turn >= kept_turns + BUILD_SLOTS)
        def _():
            out_copy(turn - BUILD_SLOTS).wait()

        fill(turn, made.at[lax.rem(turn, BUILD_SLOTS)])
        out_copy(turn).start()
        return carry

    lax.fori_loop(kept_turns, turns, spill, 0)
    for back in range(BUILD_SLOTS, 0, -1):

        @pl.when(turns - back >= kept_turns)
        def _():
            out_copy(turns - back).wait()

    degree_ref[...] = jnp.sum(degree_acc[...], axis=1)


def apply_kernel(half_bins, total_pairs, first_row, orders, kept_ref, store_ref, source_ref, out_ref, held, acc, sem):
    acc[...] = jnp.zeros_like(acc)
    rows = out_ref.shape[0]
    code_mask = 2**CODE_BITS - 1
    spans, _ = lists_of(orders, total_pairs, half_bins, first_row, first_row + rows)

    for other, order_ref in enumerate(orders):
        shift, low, high = spans[other]
        offset = other * source_ref.shape[0] // 2
        edge = jnp.minimum(high, KEPT_PAIRS - shift)
        late = jnp.maximum(low, KEPT_PAIRS - shift)

        def add(base, end, tile):
            code = order_ref[0, total_pairs + base]
            left = (code >> CODE_BITS) & code_mask
            right = code >> (2 * CODE_BITS)
            sources = jnp.concatenate(
                [source_ref[offset + left], source_ref[offset + right]], axis=1
            )
            place = jnp.where(base < end, (code & code_mask) - first_row, rows)
            acc[place] += jnp.dot(sources, tile, preferred_element_type=jnp.float32)

        def visit(turn, carry):
            for pair in range(APPLY_UNROLL // 2):
                base = low + turn * (APPLY_UNROLL // 2) + pair
                add(base, edge, kept_ref[base + shift])
            return carry

        lax.fori_loop(0, (edge - low + APPLY_UNROLL // 2 - 1) // (APPLY_UNROLL // 2), visit, 0)

        def visit_late(turn, carry):
            first = late + turn * LATE_PAIRS
            copy = pltpu.make_async_copy(
                store_ref.at[pl.ds(first + shift, LATE_PAIRS)], held, sem
            )
            copy.start()
            copy.wait()
            for pair in range(LATE_PAIRS):
                add(first + pair, high, held[pair])
            return carry

        lax.fori_loop(0, (high - late + LATE_PAIRS - 1) // LATE_PAIRS, visit_late, 0)
    out_ref[...] = acc[:rows].astype(jnp.bfloat16)


def greet(targets):
    barrier = pltpu.get_barrier_semaphore()
    for target in targets:
        pl.semaphore_signal(barrier, inc=1, device_id=target, device_id_type=MESH_ID)
    pl.semaphore_wait(barrier, len(targets))


def row_peers(n_row, side=0):
    row, col, core, chip = place_of()
    if side:
        col = chip * CORES + 1 - core
    return [(lax.rem(row + d, n_row), col) for d in range(1, n_row)]


def sibling_peers(n_col):
    row, col, _, _ = place_of()
    return [(row, lax.rem(col + CORES * d, n_col)) for d in range(1, n_col // CORES)]


def partner_of():
    row, col, core, chip = place_of()
    return (row, chip * CORES + 1 - core)


def remote(src, dst, send_sem, recv_sem, target):
    return pltpu.make_async_remote_copy(
        src_ref=src,
        dst_ref=dst,
        send_sem=send_sem,
        recv_sem=recv_sem,
        device_id=target,
        device_id_type=MESH_ID,
    )


def send(*args):
    copy = remote(*args)
    copy.start()
    return copy


def start_kernel(n_row, n_col, part, *refs):
    blocks = refs[:n_row]
    gathered_ref, root_ref, taken, theirs, roots = refs[n_row : n_row + 5]
    deg_send, deg_recv, near_send, near_recv, root_send, root_recv = refs[n_row + 5 :]
    row, col, core, chip = place_of()
    n_chip = n_col // CORES
    own = root_ref.shape[0]
    partner = partner_of()
    siblings = sibling_peers(n_col)
    mine, cross = row_peers(n_row), row_peers(n_row, 1)
    greet(siblings + mine + cross + [partner])
    copies = []
    low_half = chip < n_chip // 2
    for d, target in enumerate(siblings):
        rank = target[1] // CORES
        start = jnp.where(low_half, n_chip - 1 - rank, rank) * own
        copies.append(
            send(
                part.at[pl.ds(pl.multiple_of(start, own), own)],
                taken.at[d],
                deg_send.at[d],
                deg_recv.at[d],
                target,
            )
        )
    near = []
    for d in range(n_row):
        near.append(send(blocks[d], theirs.at[d], near_send.at[d], near_recv.at[d], partner))
    mine_rank = jnp.where(low_half, n_chip - 1 - chip, chip)
    degree = part[pl.ds(pl.multiple_of(mine_rank * own, own), own), :]
    for d, copy in enumerate(copies):
        copy.wait_recv()
        degree = degree + taken[d]
    root = lax.rsqrt(1.0 + degree)
    root_ref[...] = root
    roots[0, 0] = root
    root_copies = []
    for side, targets in ((0, mine), (1, [partner] + cross)):
        for d, target in enumerate(targets):
            d += 1 - side
            root_copies.append(
                send(roots.at[0, 0], roots.at[side, d], root_send.at[side, d], root_recv.at[side, d], target)
            )

    def scale(side, d, source, root):
        start = side * n_row * own + lax.rem(row + n_row - d, n_row) * own
        for tile in range(own):
            gathered_ref[start + tile] = (
                source[tile].astype(jnp.float32) * root[tile : tile + 1, :]
            ).astype(jnp.bfloat16)

    scale(0, 0, blocks[0], root)
    for copy in root_copies:
        copy.wait_recv()
    for d in range(1, n_row):
        scale(0, d, blocks[d], roots[0, d])
    for d in range(n_row):
        near[d].wait_recv()
        scale(1, d, theirs.at[d], roots[1, d])
    for copy in copies + near + root_copies:
        copy.wait_send()


def sum_kernel(n_row, n_col, spread, *refs):
    parts, given, refs = refs[: EARLY + 1], refs[EARLY + 1 : 2 * EARLY + 1], refs[2 * EARLY + 1 :]
    if spread:
        root_ref, hop_ref, gathered_ref, comes, goes, *sems = refs
        send_sem, recv_sem, row_send, row_recv, near_send, near_recv = sems
    else:
        root_ref, hop_ref, comes, goes, send_sem, recv_sem = refs
    row, col, core, chip = place_of()
    n_chip = n_col // CORES
    own = root_ref.shape[0]
    size = own // PIECES
    partner = partner_of()
    up = (row, lax.rem(col + CORES, n_col))
    down = (row, lax.rem(col + n_col - CORES, n_col))
    mine = row_peers(n_row)
    greet([up, down] + ([partner] + mine if spread else []))
    last = n_chip - 1
    low_half = chip < n_chip // 2
    early = jnp.where(low_half, 0, 1)
    depth = jnp.where(low_half, chip, last - chip)

    def block(rank, piece):
        if rank < EARLY:
            return parts[rank].at[piece * size : (piece + 1) * size]
        start = (rank - EARLY) * own + piece * size
        return parts[EARLY].at[start : start + size]

    def hop_copy(way, k, piece, source=None):
        return remote(
            goes.at[way, k, piece] if source is None else source,
            comes.at[way, k, piece],
            send_sem.at[way, k, piece],
            recv_sem.at[way, k, piece],
            (row, lax.rem(col + jnp.where(way == 0, CORES, n_col - CORES), n_col)),
        )

    flow = [(k, piece) for k in range(last) for piece in range(PIECES)]
    timed = [(i, 0, *f) for i, f in enumerate(flow)]
    timed += [(i + RELAY_LAG, 1, *f) for i, f in enumerate(flow) if f[0] < n_chip // 2 - 1]

    def steps():
        for _, late, k, piece in sorted(timed):
            way = 1 - early if late else early
            ahead = k < (depth if late else last - depth)
            yield k, piece, late, way, ahead

    for k, piece, late, way, ahead in steps():
        source = block(last - k if late else k, piece)

        def relay(arrived):
            goes[way, k, piece] = (
                source[...].astype(jnp.float32) + arrived.astype(jnp.float32)
            ).astype(jnp.bfloat16)
            hop_copy(way, k, piece).start()

        def relay_waited():
            hop_copy(way, k, piece).wait_recv()
            relay(comes[way, k, piece])

        if late:
            pl.when(ahead)(relay_waited)
        elif k >= EARLY:
            pl.when(ahead & (depth == 0))(lambda: hop_copy(way, k, piece, source).start())
            pl.when(ahead & (depth > 0))(relay_waited)
        else:
            pl.when(ahead & (depth == 1))(
                lambda: relay(given[k][piece * size : (piece + 1) * size])
            )
            pl.when(ahead & (depth > 1))(relay_waited)

    row_copies, near_copies = {}, {}
    for piece in range(PIECES):
        early_k = jnp.minimum(last - depth, last - 1)

        @pl.when(depth > 0)
        def _():
            hop_copy(early, early_k, piece).wait_recv()

        hop_copy(1 - early, depth, piece).wait_recv()
        start = pl.multiple_of((last - depth - EARLY) * own, own) + piece * size
        total = parts[EARLY][pl.ds(start, size)].astype(jnp.float32)
        near = comes[early, early_k, piece].astype(jnp.float32)
        total = total + jnp.where(depth > 0, near, 0.0)
        total = total + comes[1 - early, depth, piece].astype(jnp.float32)
        roots = [root_ref[piece * size + tile : piece * size + tile + 1, :] for tile in range(size)]
        if spread:
            start = row * own + piece * size
            for tile in range(size):
                gathered_ref[start + tile] = (total[tile] * (roots[tile] * roots[tile])).astype(
                    jnp.bfloat16
                )
            for d, target in enumerate(mine):
                place = gathered_ref.at[pl.ds(start, size)]
                row_copies[piece, d] = send(
                    place, place, row_send.at[piece, d], row_recv.at[piece, d], target
                )
            near_copies[piece, 0] = send(
                gathered_ref.at[pl.ds(start, size)],
                gathered_ref.at[pl.ds(n_row * own + start, size)],
                near_send.at[piece, 0],
                near_recv.at[piece, 0],
                partner,
            )
        for tile in range(size):
            place = (piece * size + tile) * TILE
            hop_ref[place : place + TILE, :] = (total[tile] * roots[tile]).T.astype(jnp.bfloat16)
    for (piece, d), copy in row_copies.items():
        copy.wait_recv()
        start = lax.rem(row + n_row - d - 1, n_row) * own + piece * size
        near_copies[piece, d + 1] = send(
            gathered_ref.at[pl.ds(start, size)],
            gathered_ref.at[pl.ds(n_row * own + start, size)],
            near_send.at[piece, d + 1],
            near_recv.at[piece, d + 1],
            partner,
        )
    for copy in near_copies.values():
        copy.wait_recv()
    for copy in list(row_copies.values()) + list(near_copies.values()):
        copy.wait_send()
    for k, piece, late, way, ahead in steps():
        if not late and k < EARLY:
            ahead = ahead & (depth > 0)
        pl.when(ahead)(lambda: hop_copy(way, k, piece).wait_send())


def sems(*shape):
    return pltpu.SemaphoreType.DMA(shape)


def comm_params(ident, scratch):
    return pltpu.CompilerParams(
        collective_id=ident, has_side_effects=True, vmem_limit_bytes=scratch + 2**20
    )


def full_params():
    return pltpu.CompilerParams(vmem_limit_bytes=67043328)


def plain_params(scratch):
    return pltpu.CompilerParams(vmem_limit_bytes=scratch + 2**20)


def local(features, tile_rows, tile_cols, edge_lists, tile_counts):
    node_count, feat_width = features.shape
    n_row, n_col = lax.axis_size("row"), lax.axis_size("col")
    n_chip = n_col // CORES
    own = node_count // TILE
    half_tiles = own * n_chip
    source_tiles = own * n_row
    slots = tile_rows.shape[-1]
    bf16, f32 = jnp.bfloat16, jnp.float32
    tile_bytes = feat_width * TILE * 2
    spare = max(BUILD_UNROLL, APPLY_UNROLL)
    pairs = -(-(slots + CORES * half_tiles + spare) // (2 * TILE)) * TILE
    swap = [(i, i + 1 - 2 * (i % CORES)) for i in range(n_col)]
    edges = edge_lists.reshape(2, slots, TILE)

    edges_b = lax.ppermute(edges, "col", swap)
    codes = 2 * pairs + -(-(CORES * half_tiles) // TILE) * TILE + TILE
    order, turned = pl.pallas_call(
        functools.partial(order_kernel, own, n_chip, pairs),
        out_shape=[
            jax.ShapeDtypeStruct((1, codes), jnp.int32),
            jax.ShapeDtypeStruct((own, feat_width, TILE), bf16),
        ],
        in_specs=[SMEM_SPEC] + [HBM_SPEC] * 3,
        out_specs=[VMEM_SPEC] * 2,
        scratch_shapes=[
            pltpu.VMEM((1, slots), jnp.int32),
            pltpu.VMEM((1, slots), jnp.int32),
            pltpu.VMEM((node_count, feat_width), bf16),
            sems(3),
        ],
        compiler_params=full_params(),
        name="order",
    )(tile_counts[0], tile_rows[0], tile_cols[0], features)
    blocks = [turned] + [
        lax.ppermute(turned, "row", [(i, (i + d) % n_row) for i in range(n_row)])
        for d in range(1, n_row)
    ]
    order_b = lax.ppermute(order, "col", swap)

    kept, store, degree = pl.pallas_call(
        functools.partial(build_kernel, half_tiles, pairs),
        in_specs=[SMEM_SPEC] * 2 + [HBM_SPEC] * 2,
        out_specs=[VMEM_SPEC, ANY_SPEC, VMEM_SPEC],
        scratch_shapes=[
            pltpu.VMEM((2, 2, slots, TILE), jnp.int32),
            pltpu.VMEM((BUILD_SLOTS, BUILD_UNROLL // 2, 2 * TILE, TILE), bf16),
            pltpu.VMEM((half_tiles, 8, TILE), f32),
            sems(BUILD_SLOTS),
            sems(2),
        ],
        out_shape=[
            jax.ShapeDtypeStruct((KEPT_PAIRS + APPLY_UNROLL // 2, 2 * TILE, TILE), bf16),
            jax.ShapeDtypeStruct((2 * pairs, 2 * TILE, TILE), bf16),
            jax.ShapeDtypeStruct((half_tiles, TILE), f32),
        ],
        compiler_params=plain_params(4 * slots * TILE * 4 + BUILD_UNROLL * TILE * TILE * 2),
        cost_estimate=pl.CostEstimate(flops=10**10, bytes_accessed=0, transcendentals=0),
        name="build",
    )(order, order_b, edges, edges_b)

    gathered_type = jax.ShapeDtypeStruct((CORES * source_tiles, feat_width, TILE), bf16)
    gathered, root = pl.pallas_call(
        functools.partial(start_kernel, n_row, n_col),
        out_shape=[gathered_type, jax.ShapeDtypeStruct((own, TILE), f32)],
        in_specs=[VMEM_SPEC] * (1 + n_row),
        out_specs=[VMEM_SPEC] * 2,
        scratch_shapes=[
            pltpu.VMEM((n_chip - 1, own, TILE), f32),
            pltpu.VMEM((n_row, own, feat_width, TILE), bf16),
            pltpu.VMEM((2, n_row, own, TILE), f32),
            sems(n_chip - 1),
            sems(n_chip - 1),
            sems(n_row),
            sems(n_row),
            sems(2, n_row),
            sems(2, n_row),
        ],
        compiler_params=comm_params(0, n_row * own * tile_bytes),
        name="start",
    )(degree, *blocks)

    def apply(sources, ranks, after, hop=None):
        rows = len(ranks) * own
        hops = [] if hop is None else [hop]

        def body(order_a, order_b, kept, store, sources, after, *refs):
            if hops:
                hop_ref, out_ref, hop_out, *scratch, hop_sem = refs
                copy = pltpu.make_async_copy(hop_ref, hop_out, hop_sem)
                copy.start()
            else:
                out_ref, *scratch = refs
            apply_kernel(
                half_tiles,
                pairs,
                ranks[0] * own,
                (order_a, order_b),
                kept,
                store,
                sources,
                out_ref,
                *scratch,
            )
            if hops:
                copy.wait()

        return pl.pallas_call(
            body,
            in_specs=[SMEM_SPEC] * 2
            + [VMEM_SPEC, ANY_SPEC] * 2
            + [VMEM_SPEC] * len(hops),
            out_specs=[VMEM_SPEC] + [ANY_SPEC] * len(hops),
            scratch_shapes=[
                pltpu.VMEM((LATE_PAIRS, 2 * TILE, TILE), bf16),
                pltpu.VMEM((rows + 1, feat_width, TILE), f32),
                pltpu.SemaphoreType.DMA,
            ]
            + [pltpu.SemaphoreType.DMA] * len(hops),
            out_shape=[jax.ShapeDtypeStruct((rows, feat_width, TILE), bf16)]
            + [jax.ShapeDtypeStruct(hop.shape, hop.dtype) for hop in hops],
            compiler_params=plain_params((2 * rows + 2 + 2 * LATE_PAIRS) * tile_bytes),
            cost_estimate=pl.CostEstimate(flops=10**10, bytes_accessed=0, transcendentals=0),
            name="apply",
        )(order, order_b, kept, store, sources, after, *hops)

    ends = [
        (a * CORES + core, b * CORES + core)
        for a, b in ((0, 1), (n_chip - 1, n_chip - 2))
        for core in range(CORES)
    ]

    def apply_all(sources, hop=None):
        parts, given, after = [], [], sources
        for rank in range(EARLY):
            (part,) = apply(sources, [rank], after)
            parts.append(part)
            given.append(lax.ppermute(part, "col", ends))
            after = part
        part, *hops = apply(sources, list(range(EARLY, n_chip)), after, hop)
        return parts + [part] + given, *hops

    def collect(parts, spread):
        size = own // PIECES
        outs = [jax.ShapeDtypeStruct((node_count, feat_width), bf16)]
        semaphores = [sems(2, n_chip - 1, PIECES)] * 2
        if spread:
            outs.append(gathered_type)
            semaphores += [sems(PIECES, n_row - 1)] * 2 + [sems(PIECES, n_row)] * 2
        return pl.pallas_call(
            functools.partial(sum_kernel, n_row, n_col, spread),
            out_shape=outs,
            in_specs=[VMEM_SPEC] * (len(parts) + 1),
            out_specs=[VMEM_SPEC] * len(outs),
            scratch_shapes=[pltpu.VMEM((2, n_chip - 1, PIECES, size, feat_width, TILE), bf16)] * 2
            + semaphores,
            compiler_params=comm_params(
                1 if spread else 2, 4 * (n_chip - 1) * own * tile_bytes
            ),
            name="spread" if spread else "finish",
        )(*parts, root)

    (parts,) = apply_all(gathered)
    hop_one, gathered = collect(parts, True)
    parts, hop_one = apply_all(gathered, hop_one)
    (hop_two,) = collect(parts, False)
    return (hop_one, hop_two)


def solution(mesh):
    placed = (
        P(("row", "col"), None),
        P("row", "col", None),
        P("row", "col", None),
        P(None, "row", "col", None, None),
        P("row", "col"),
    )
    return jax.shard_map(
        local,
        mesh=mesh,
        in_specs=placed,
        out_specs=(P(("row", "col"), None), P(("row", "col"), None)),
        check_vma=False,
    )
```

```python
import functools

import jax
import jax.numpy as jnp
from jax import lax
from jax.experimental import pallas as pl
from jax.experimental.pallas import tpu as pltpu
from jax.sharding import PartitionSpec as P

TILE = 128
ROWS_MIN = 16
BUILD_UNROLL = 32
BUILD_SLOTS = 1
KEPT_PAIRS = 416
LATE_PAIRS = 8
APPLY_UNROLL = 64
APPLY_SLOTS = 4
HOT = jnp.float8_e4m3fn
HOT_ROWS = 32
EXTRA = 16
SLOT_BITS = 11
CODE_BITS = 8
PIECES = 8
RELAY_LAG = 5
EARLY = 1
CORES = 2
MESH_ID = pl.DeviceIdType.MESH
VMEM_SPEC = pl.BlockSpec(memory_space=pltpu.VMEM)
SMEM_SPEC = pl.BlockSpec(memory_space=pltpu.SMEM)
ANY_SPEC = pl.BlockSpec(memory_space=pl.ANY)
HBM_SPEC = pl.BlockSpec(memory_space=pltpu.HBM)


def place_of():
    row, col = lax.axis_index("row"), lax.axis_index("col")
    return row, col, lax.rem(col, CORES), col // CORES


def order_kernel(own, n_chip, pairs, count_ref, rows_ref, cols_ref, order_ref):
    slots = rows_ref.shape[-1]
    bins = CORES * n_chip * own
    bf16, f32 = jnp.bfloat16, jnp.float32
    _, _, core, chip = place_of()

    def iota(shape, dim):
        return lax.broadcasted_iota(jnp.int32, shape, dim)

    def hot(mask):
        return jnp.where(mask, 1.0, 0.0).astype(bf16)

    def mul(x, y):
        return jnp.dot(x.astype(bf16), y.astype(bf16), preferred_element_type=f32)

    slot = iota((1, slots), 1)
    alive = slot < count_ref[0, 0]
    rows = jnp.where(alive, rows_ref[...], 0)
    cols = jnp.where(alive, cols_ref[...], 0)
    owner = rows // own
    target = owner // CORES
    other = jnp.where(lax.rem(owner, CORES) == core, 0, 1)
    rank = jnp.where(chip < n_chip // 2, n_chip - 1 - target, target)
    local = rank * own + lax.rem(rows, own)
    bin_of = jnp.where(alive, other * n_chip * own + local, -1)
    belongs = bin_of == iota((bins, slots), 0)
    ranks = mul(hot(belongs), hot(iota((slots, slots), 0) <= iota((slots, slots), 1)))
    totals = jnp.broadcast_to(ranks[:, slots - 1 :], (bins, TILE)).astype(jnp.int32)
    halves = (totals + 1) // 2
    before = hot(iota((bins, bins), 1) < iota((bins, bins), 0))
    offsets = 32.0 * mul(before, (halves // 32).astype(f32)) + mul(before, (halves % 32).astype(f32))
    spots = jnp.where(belongs, ranks - 1.0 + 2.0 * offsets[:, :1], 0.0)
    spot = jnp.where(alive, jnp.sum(spots, axis=0, keepdims=True), -1.0)
    odd = jnp.where(alive, spot.astype(jnp.int32) % 2, -1)
    facts = []
    for side in range(2):
        here = odd == side
        facts += [
            jnp.where(here, fact, 0)
            for fact in (slot // 32, slot % 32, jnp.where(here, 1, 0), cols, local)
        ]
    facts = jnp.concatenate(
        [fact.astype(f32) for fact in facts] + [jnp.zeros((EXTRA - len(facts), slots), f32)], axis=0
    )
    pair_of = jnp.broadcast_to(spot, (TILE, slots)).T.astype(jnp.int32) >> 1
    for start in range(0, pairs, TILE):
        found = mul(facts, hot(pair_of == iota((slots, TILE), 1) + start)).astype(jnp.int32)
        places = [32 * found[i : i + 1] + found[i + 1 : i + 2] + found[i + 2 : i + 3] for i in (0, 5)]
        row, cols = found[4:5], (found[3:4], found[8:9])
        order_ref[:, start : start + TILE] = (row << (2 * SLOT_BITS)) + (places[1] << SLOT_BITS) + places[0]
        order_ref[:, pairs + start : pairs + start + TILE] = (
            (cols[1] << (2 * CODE_BITS)) + (cols[0] << CODE_BITS) + row
        )
    end = jnp.sum(halves.astype(f32), axis=0, keepdims=True).astype(jnp.int32)
    order_ref[:, 2 * pairs : 2 * pairs + bins] = offsets.T[0:1, :].astype(jnp.int32)
    order_ref[:, 2 * pairs + bins : 2 * pairs + bins + TILE] = end


def spans_of(order_ref, pairs, half_bins, other, first, last):
    base = 2 * pairs + other * half_bins
    return order_ref[0, base], order_ref[0, base + first], order_ref[0, base + last]


def lists_of(orders, total_pairs, half_bins, first, last):
    pairs = BUILD_UNROLL // 2
    spans, start = [], 0
    for other, order_ref in enumerate(orders):
        low, begin, end = spans_of(order_ref, total_pairs, half_bins, other, first, last)
        spans.append((start - low, begin, end))
        high = spans_of(order_ref, total_pairs, half_bins, other, 0, half_bins)[2]
        start = start + (high - low + pairs - 1) // pairs * pairs
    return spans, start // pairs


def build_kernel(
    half_bins, total_pairs, order_a, order_b, edges_a, edges_b, kept_ref, store_ref, degree_ref,
    edges_ref, made, degree_acc, sem, edge_sem
):
    loads = [
        pltpu.make_async_copy(source, edges_ref.at[i], edge_sem.at[i])
        for i, source in enumerate((edges_a, edges_b))
    ]
    for load in loads:
        load.start()
    degree_acc[...] = jnp.zeros_like(degree_acc)
    pairs = BUILD_UNROLL // 2
    (span_a, span_b), turns = lists_of((order_a, order_b), total_pairs, half_bins, 0, half_bins)
    turns_a = (span_b[0] + span_b[1]) // pairs
    kept_turns = jnp.minimum(turns, KEPT_PAIRS // pairs)
    mask = 2**SLOT_BITS - 1
    cells = [
        (lax.broadcasted_iota(jnp.int32, (HOT_ROWS, TILE), 0) + start).astype(jnp.int8)
        for start in range(0, TILE, HOT_ROWS)
    ]

    def hot(ids):
        ids = jnp.broadcast_to(ids, (HOT_ROWS, TILE)).astype(jnp.int8)
        return jnp.concatenate(
            [jnp.where(ids == cell, HOT(1), HOT(0)) for cell in cells], axis=0
        )

    def fill(turn, target):
        mine = turn < turns_a
        other = jnp.where(mine, 0, 1)
        high = jnp.where(mine, span_a[2], span_b[2])
        low = turn * pairs - jnp.where(mine, 0, span_b[0])
        for pair in range(pairs):
            counts = []
            base = low + pair
            code = jnp.where(mine, order_a[0, base], order_b[0, base])
            live = jnp.where(base < high, code, 0)
            for half in range(2):
                slot = ((live >> (half * SLOT_BITS)) & mask) - 1
                safe = jnp.maximum(slot, 0)
                dst = jnp.where(slot >= 0, edges_ref[other, 0, pl.ds(safe, 1), :], -1)
                src = edges_ref[other, 1, pl.ds(safe, 1), :]
                both = lax.dot_general(
                    hot(src), hot(dst), (((1,), (1,)), ((), ())), preferred_element_type=jnp.float32
                )
                target[pair, half * TILE : (half + 1) * TILE] = both.astype(jnp.bfloat16)
                counts.append(jnp.sum(both.reshape(TILE // 8, 8, TILE), axis=0))
            degree_acc[live >> (2 * SLOT_BITS)] += counts[0] + counts[1]

    def keep(turn, carry):
        fill(turn, kept_ref.at[pl.ds(turn * pairs, pairs)])
        return carry

    for load in loads:
        load.wait()
    lax.fori_loop(0, kept_turns, keep, 0)

    def out_copy(turn):
        side = lax.rem(turn, BUILD_SLOTS)
        return pltpu.make_async_copy(
            made.at[side], store_ref.at[pl.ds(turn * pairs, pairs)], sem.at[side]
        )

    def spill(turn, carry):
        @pl.when(turn >= kept_turns + BUILD_SLOTS)
        def _():
            out_copy(turn - BUILD_SLOTS).wait()

        fill(turn, made.at[lax.rem(turn, BUILD_SLOTS)])
        out_copy(turn).start()
        return carry

    lax.fori_loop(kept_turns, turns, spill, 0)
    for back in range(BUILD_SLOTS, 0, -1):

        @pl.when(turns - back >= kept_turns)
        def _():
            out_copy(turns - back).wait()

    degree_ref[...] = jnp.sum(degree_acc[...], axis=1)


def apply_kernel(half_bins, total_pairs, first_row, orders, kept_ref, store_ref, source_ref, out_ref, held, acc, sem):
    acc[...] = jnp.zeros_like(acc)
    rows = out_ref.shape[0]
    code_mask = 2**CODE_BITS - 1
    spans, _ = lists_of(orders, total_pairs, half_bins, first_row, first_row + rows)

    for other, order_ref in enumerate(orders):
        shift, low, high = spans[other]
        offset = other * source_ref.shape[0] // 2
        edge = jnp.minimum(high, KEPT_PAIRS - shift)
        late = jnp.maximum(low, KEPT_PAIRS - shift)

        def add(base, end, tile):
            code = order_ref[0, total_pairs + base]
            left = (code >> CODE_BITS) & code_mask
            right = code >> (2 * CODE_BITS)
            sources = jnp.concatenate(
                [source_ref[offset + left], source_ref[offset + right]], axis=1
            )
            place = jnp.where(base < end, (code & code_mask) - first_row, rows)
            acc[place] += jnp.dot(sources, tile, preferred_element_type=jnp.float32)

        def visit(turn, carry):
            for pair in range(APPLY_UNROLL // 2):
                base = low + turn * (APPLY_UNROLL // 2) + pair
                add(base, edge, kept_ref[base + shift])
            return carry

        lax.fori_loop(0, (edge - low + APPLY_UNROLL // 2 - 1) // (APPLY_UNROLL // 2), visit, 0)

        def visit_late(turn, carry):
            first = late + turn * LATE_PAIRS
            copy = pltpu.make_async_copy(
                store_ref.at[pl.ds(first + shift, LATE_PAIRS)], held, sem
            )
            copy.start()
            copy.wait()
            for pair in range(LATE_PAIRS):
                add(first + pair, high, held[pair])
            return carry

        lax.fori_loop(0, (high - late + LATE_PAIRS - 1) // LATE_PAIRS, visit_late, 0)
    out_ref[...] = acc[:rows].astype(jnp.bfloat16)


def greet(targets):
    barrier = pltpu.get_barrier_semaphore()
    for target in targets:
        pl.semaphore_signal(barrier, inc=1, device_id=target, device_id_type=MESH_ID)
    pl.semaphore_wait(barrier, len(targets))


def row_peers(n_row, side=0):
    row, col, core, chip = place_of()
    if side:
        col = chip * CORES + 1 - core
    return [(lax.rem(row + d, n_row), col) for d in range(1, n_row)]


def sibling_peers(n_col):
    row, col, _, _ = place_of()
    return [(row, lax.rem(col + CORES * d, n_col)) for d in range(1, n_col // CORES)]


def partner_of():
    row, col, core, chip = place_of()
    return (row, chip * CORES + 1 - core)


def remote(src, dst, send_sem, recv_sem, target):
    return pltpu.make_async_remote_copy(
        src_ref=src,
        dst_ref=dst,
        send_sem=send_sem,
        recv_sem=recv_sem,
        device_id=target,
        device_id_type=MESH_ID,
    )


def send(*args):
    copy = remote(*args)
    copy.start()
    return copy


def start_kernel(n_row, n_col, part, *refs):
    blocks = refs[:n_row]
    gathered_ref, root_ref, taken, theirs, roots = refs[n_row : n_row + 5]
    deg_send, deg_recv, near_send, near_recv, root_send, root_recv = refs[n_row + 5 :]
    row, col, core, chip = place_of()
    n_chip = n_col // CORES
    own = root_ref.shape[0]
    partner = partner_of()
    siblings = sibling_peers(n_col)
    mine, cross = row_peers(n_row), row_peers(n_row, 1)
    greet(siblings + mine + cross + [partner])
    copies = []
    low_half = chip < n_chip // 2
    for d, target in enumerate(siblings):
        rank = target[1] // CORES
        start = jnp.where(low_half, n_chip - 1 - rank, rank) * own
        copies.append(
            send(
                part.at[pl.ds(pl.multiple_of(start, own), own)],
                taken.at[d],
                deg_send.at[d],
                deg_recv.at[d],
                target,
            )
        )
    near = []
    for d in range(n_row):
        near.append(send(blocks[d], theirs.at[d], near_send.at[d], near_recv.at[d], partner))
    mine_rank = jnp.where(low_half, n_chip - 1 - chip, chip)
    def start_of(side, d):
        return side * n_row * own + lax.rem(row + n_row - d, n_row) * own

    def turn(side, d, source):
        for tile in range(own):
            block = source[tile * TILE : (tile + 1) * TILE, :].astype(jnp.float32).T
            gathered_ref[start_of(side, d) + tile] = block.astype(jnp.bfloat16)

    for d in range(n_row):
        turn(0, d, blocks[d])
    degree = part[pl.ds(pl.multiple_of(mine_rank * own, own), own), :]
    for d, copy in enumerate(copies):
        copy.wait_recv()
        degree = degree + taken[d]
    root = lax.rsqrt(1.0 + degree)
    root_ref[...] = root
    roots[0, 0] = root
    root_copies = []
    for side, targets in ((0, mine), (1, [partner] + cross)):
        for d, target in enumerate(targets):
            d += 1 - side
            root_copies.append(
                send(roots.at[0, 0], roots.at[side, d], root_send.at[side, d], root_recv.at[side, d], target)
            )

    def scale(side, d, root):
        for tile in range(own):
            place = start_of(side, d) + tile
            gathered_ref[place] = (
                gathered_ref[place].astype(jnp.float32) * root[tile : tile + 1, :]
            ).astype(jnp.bfloat16)

    for d in range(n_row):
        near[d].wait_recv()
        turn(1, d, theirs.at[d])
    scale(0, 0, root)
    for copy in root_copies:
        copy.wait_recv()
    for side in range(2):
        for d in range(1 - side, n_row):
            scale(side, d, roots[side, d])
    for copy in copies + near + root_copies:
        copy.wait_send()


def sum_kernel(n_row, n_col, spread, *refs):
    parts, given, refs = refs[: EARLY + 1], refs[EARLY + 1 : 2 * EARLY + 1], refs[2 * EARLY + 1 :]
    if spread:
        root_ref, hop_ref, gathered_ref, comes, goes, *sems = refs
        send_sem, recv_sem, row_send, row_recv, near_send, near_recv = sems
    else:
        root_ref, hop_ref, comes, goes, send_sem, recv_sem = refs
    row, col, core, chip = place_of()
    n_chip = n_col // CORES
    own = root_ref.shape[0]
    size = own // PIECES
    partner = partner_of()
    up = (row, lax.rem(col + CORES, n_col))
    down = (row, lax.rem(col + n_col - CORES, n_col))
    mine = row_peers(n_row)
    greet([up, down] + ([partner] + mine if spread else []))
    last = n_chip - 1
    low_half = chip < n_chip // 2
    early = jnp.where(low_half, 0, 1)
    depth = jnp.where(low_half, chip, last - chip)

    def block(rank, piece):
        if rank < EARLY:
            return parts[rank].at[piece * size : (piece + 1) * size]
        start = (rank - EARLY) * own + piece * size
        return parts[EARLY].at[start : start + size]

    def hop_copy(way, k, piece, source=None):
        return remote(
            goes.at[way, k, piece] if source is None else source,
            comes.at[way, k, piece],
            send_sem.at[way, k, piece],
            recv_sem.at[way, k, piece],
            (row, lax.rem(col + jnp.where(way == 0, CORES, n_col - CORES), n_col)),
        )

    flow = [(k, piece) for k in range(last) for piece in range(PIECES)]
    timed = [(i, 0, *f) for i, f in enumerate(flow)]
    timed += [(i + RELAY_LAG, 1, *f) for i, f in enumerate(flow) if f[0] < n_chip // 2 - 1]

    def steps():
        for _, late, k, piece in sorted(timed):
            way = 1 - early if late else early
            ahead = k < (depth if late else last - depth)
            yield k, piece, late, way, ahead

    for k, piece, late, way, ahead in steps():
        source = block(last - k if late else k, piece)

        def relay(arrived):
            goes[way, k, piece] = (
                source[...].astype(jnp.float32) + arrived.astype(jnp.float32)
            ).astype(jnp.bfloat16)
            hop_copy(way, k, piece).start()

        def relay_waited():
            hop_copy(way, k, piece).wait_recv()
            relay(comes[way, k, piece])

        if late:
            pl.when(ahead)(relay_waited)
        elif k >= EARLY:
            pl.when(ahead & (depth == 0))(lambda: hop_copy(way, k, piece, source).start())
            pl.when(ahead & (depth > 0))(relay_waited)
        else:
            pl.when(ahead & (depth == 1))(
                lambda: relay(given[k][piece * size : (piece + 1) * size])
            )
            pl.when(ahead & (depth > 1))(relay_waited)

    row_copies, near_copies = {}, {}
    for piece in range(PIECES):
        early_k = jnp.minimum(last - depth, last - 1)

        @pl.when(depth > 0)
        def _():
            hop_copy(early, early_k, piece).wait_recv()

        hop_copy(1 - early, depth, piece).wait_recv()
        start = pl.multiple_of((last - depth - EARLY) * own, own) + piece * size
        total = parts[EARLY][pl.ds(start, size)].astype(jnp.float32)
        near = comes[early, early_k, piece].astype(jnp.float32)
        total = total + jnp.where(depth > 0, near, 0.0)
        total = total + comes[1 - early, depth, piece].astype(jnp.float32)
        roots = [root_ref[piece * size + tile : piece * size + tile + 1, :] for tile in range(size)]
        if spread:
            start = row * own + piece * size
            for tile in range(size):
                gathered_ref[start + tile] = (total[tile] * (roots[tile] * roots[tile])).astype(
                    jnp.bfloat16
                )
            for d, target in enumerate(mine):
                place = gathered_ref.at[pl.ds(start, size)]
                row_copies[piece, d] = send(
                    place, place, row_send.at[piece, d], row_recv.at[piece, d], target
                )
            near_copies[piece, 0] = send(
                gathered_ref.at[pl.ds(start, size)],
                gathered_ref.at[pl.ds(n_row * own + start, size)],
                near_send.at[piece, 0],
                near_recv.at[piece, 0],
                partner,
            )
        for tile in range(size):
            place = (piece * size + tile) * TILE
            hop_ref[place : place + TILE, :] = (total[tile] * roots[tile]).T.astype(jnp.bfloat16)
    for (piece, d), copy in row_copies.items():
        copy.wait_recv()
        start = lax.rem(row + n_row - d - 1, n_row) * own + piece * size
        near_copies[piece, d + 1] = send(
            gathered_ref.at[pl.ds(start, size)],
            gathered_ref.at[pl.ds(n_row * own + start, size)],
            near_send.at[piece, d + 1],
            near_recv.at[piece, d + 1],
            partner,
        )
    for copy in near_copies.values():
        copy.wait_recv()
    for copy in list(row_copies.values()) + list(near_copies.values()):
        copy.wait_send()
    for k, piece, late, way, ahead in steps():
        if not late and k < EARLY:
            ahead = ahead & (depth > 0)
        pl.when(ahead)(lambda: hop_copy(way, k, piece).wait_send())


def sems(*shape):
    return pltpu.SemaphoreType.DMA(shape)


def comm_params(ident, scratch):
    return pltpu.CompilerParams(
        collective_id=ident, has_side_effects=True, vmem_limit_bytes=scratch + 2**20
    )


def full_params():
    return pltpu.CompilerParams(vmem_limit_bytes=67043328)


def plain_params(scratch):
    return pltpu.CompilerParams(vmem_limit_bytes=scratch + 2**20)


def local(features, tile_rows, tile_cols, edge_lists, tile_counts):
    node_count, feat_width = features.shape
    n_row, n_col = lax.axis_size("row"), lax.axis_size("col")
    n_chip = n_col // CORES
    own = node_count // TILE
    half_tiles = own * n_chip
    source_tiles = own * n_row
    slots = tile_rows.shape[-1]
    bf16, f32 = jnp.bfloat16, jnp.float32
    tile_bytes = feat_width * TILE * 2
    spare = max(BUILD_UNROLL, APPLY_UNROLL)
    pairs = -(-(slots + CORES * half_tiles + spare) // (2 * TILE)) * TILE
    swap = [(i, i + 1 - 2 * (i % CORES)) for i in range(n_col)]
    edges = edge_lists.reshape(2, slots, TILE)

    blocks = [features] + [
        lax.ppermute(features, "row", [(i, (i + d) % n_row) for i in range(n_row)])
        for d in range(1, n_row)
    ]
    edges_b = lax.ppermute(edges, "col", swap)
    codes = 2 * pairs + -(-(CORES * half_tiles) // TILE) * TILE + TILE
    order = pl.pallas_call(
        functools.partial(order_kernel, own, n_chip, pairs),
        out_shape=jax.ShapeDtypeStruct((1, codes), jnp.int32),
        in_specs=[SMEM_SPEC] + [VMEM_SPEC] * 2,
        out_specs=VMEM_SPEC,
        compiler_params=plain_params(16 * 2**20),
        cost_estimate=pl.CostEstimate(flops=10**10, bytes_accessed=0, transcendentals=0),
        name="order",
    )(tile_counts, tile_rows[0], tile_cols[0])
    order_b = lax.ppermute(order, "col", swap)

    kept, store, degree = pl.pallas_call(
        functools.partial(build_kernel, half_tiles, pairs),
        in_specs=[SMEM_SPEC] * 2 + [HBM_SPEC] * 2,
        out_specs=[VMEM_SPEC, ANY_SPEC, VMEM_SPEC],
        scratch_shapes=[
            pltpu.VMEM((2, 2, slots, TILE), jnp.int32),
            pltpu.VMEM((BUILD_SLOTS, BUILD_UNROLL // 2, 2 * TILE, TILE), bf16),
            pltpu.VMEM((half_tiles, 8, TILE), f32),
            sems(BUILD_SLOTS),
            sems(2),
        ],
        out_shape=[
            jax.ShapeDtypeStruct((KEPT_PAIRS + APPLY_UNROLL // 2, 2 * TILE, TILE), bf16),
            jax.ShapeDtypeStruct((2 * pairs, 2 * TILE, TILE), bf16),
            jax.ShapeDtypeStruct((half_tiles, TILE), f32),
        ],
        compiler_params=plain_params(4 * slots * TILE * 4 + BUILD_UNROLL * TILE * TILE * 2),
        name="build",
    )(order, order_b, edges, edges_b)

    gathered_type = jax.ShapeDtypeStruct((CORES * source_tiles, feat_width, TILE), bf16)
    gathered, root = pl.pallas_call(
        functools.partial(start_kernel, n_row, n_col),
        out_shape=[gathered_type, jax.ShapeDtypeStruct((own, TILE), f32)],
        in_specs=[VMEM_SPEC] * (1 + n_row),
        out_specs=[VMEM_SPEC] * 2,
        scratch_shapes=[
            pltpu.VMEM((n_chip - 1, own, TILE), f32),
            pltpu.VMEM((n_row, node_count, feat_width), bf16),
            pltpu.VMEM((2, n_row, own, TILE), f32),
            sems(n_chip - 1),
            sems(n_chip - 1),
            sems(n_row),
            sems(n_row),
            sems(2, n_row),
            sems(2, n_row),
        ],
        compiler_params=comm_params(0, n_row * own * tile_bytes),
        name="start",
    )(degree, *blocks)

    def apply(sources, ranks, after, hop=None):
        rows = len(ranks) * own
        hops = [] if hop is None else [hop]

        def body(order_a, order_b, kept, store, sources, after, *refs):
            if hops:
                hop_ref, out_ref, hop_out, *scratch, hop_sem = refs
                copy = pltpu.make_async_copy(hop_ref, hop_out, hop_sem)
                copy.start()
            else:
                out_ref, *scratch = refs
            apply_kernel(
                half_tiles,
                pairs,
                ranks[0] * own,
                (order_a, order_b),
                kept,
                store,
                sources,
                out_ref,
                *scratch,
            )
            if hops:
                copy.wait()

        return pl.pallas_call(
            body,
            in_specs=[SMEM_SPEC] * 2
            + [VMEM_SPEC, ANY_SPEC] * 2
            + [VMEM_SPEC] * len(hops),
            out_specs=[VMEM_SPEC] + [ANY_SPEC] * len(hops),
            scratch_shapes=[
                pltpu.VMEM((LATE_PAIRS, 2 * TILE, TILE), bf16),
                pltpu.VMEM((rows + 1, feat_width, TILE), f32),
                pltpu.SemaphoreType.DMA,
            ]
            + [pltpu.SemaphoreType.DMA] * len(hops),
            out_shape=[jax.ShapeDtypeStruct((rows, feat_width, TILE), bf16)]
            + [jax.ShapeDtypeStruct(hop.shape, hop.dtype) for hop in hops],
            compiler_params=plain_params((2 * rows + 2 + 2 * LATE_PAIRS) * tile_bytes),
            cost_estimate=pl.CostEstimate(flops=10**10, bytes_accessed=0, transcendentals=0),
            name="apply",
        )(order, order_b, kept, store, sources, after, *hops)

    ends = [
        (a * CORES + core, b * CORES + core)
        for a, b in ((0, 1), (n_chip - 1, n_chip - 2))
        for core in range(CORES)
    ]

    def apply_all(sources, hop=None):
        parts, given, after = [], [], sources
        for rank in range(EARLY):
            (part,) = apply(sources, [rank], after)
            parts.append(part)
            given.append(lax.ppermute(part, "col", ends))
            after = part
        part, *hops = apply(sources, list(range(EARLY, n_chip)), after, hop)
        return parts + [part] + given, *hops

    def collect(parts, spread):
        size = own // PIECES
        outs = [jax.ShapeDtypeStruct((node_count, feat_width), bf16)]
        semaphores = [sems(2, n_chip - 1, PIECES)] * 2
        if spread:
            outs.append(gathered_type)
            semaphores += [sems(PIECES, n_row - 1)] * 2 + [sems(PIECES, n_row)] * 2
        return pl.pallas_call(
            functools.partial(sum_kernel, n_row, n_col, spread),
            out_shape=outs,
            in_specs=[VMEM_SPEC] * (len(parts) + 1),
            out_specs=[VMEM_SPEC] * len(outs),
            scratch_shapes=[pltpu.VMEM((2, n_chip - 1, PIECES, size, feat_width, TILE), bf16)] * 2
            + semaphores,
            compiler_params=comm_params(
                1 if spread else 2, 4 * (n_chip - 1) * own * tile_bytes
            ),
            name="spread" if spread else "finish",
        )(*parts, root)

    (parts,) = apply_all(gathered)
    hop_one, gathered = collect(parts, True)
    parts, hop_one = apply_all(gathered, hop_one)
    (hop_two,) = collect(parts, False)
    return (hop_one, hop_two)


def solution(mesh):
    placed = (
        P(("row", "col"), None),
        P("row", "col", None),
        P("row", "col", None),
        P(None, "row", "col", None, None),
        P("row", "col"),
    )
    return jax.shard_map(
        local,
        mesh=mesh,
        in_specs=placed,
        out_specs=(P(("row", "col"), None), P(("row", "col"), None)),
        check_vma=False,
    )
```

```python
import functools

import jax
import jax.numpy as jnp
from jax import lax
from jax.experimental import pallas as pl
from jax.experimental.pallas import tpu as pltpu
from jax.sharding import PartitionSpec as P

TILE = 128
ROWS_MIN = 16
BUILD_UNROLL = 32
BUILD_SLOTS = 1
KEPT_PAIRS = 416
LATE_PAIRS = 8
APPLY_UNROLL = 64
APPLY_SLOTS = 4
HOT = jnp.float8_e4m3fn
HOT_ROWS = 32
EXTRA = 16
SLOT_BITS = 11
CODE_BITS = 8
PIECES = 4
RELAY_LAG = 3
EARLY = 1
CORES = 2
MESH_ID = pl.DeviceIdType.MESH
VMEM_SPEC = pl.BlockSpec(memory_space=pltpu.VMEM)
SMEM_SPEC = pl.BlockSpec(memory_space=pltpu.SMEM)
ANY_SPEC = pl.BlockSpec(memory_space=pl.ANY)
HBM_SPEC = pl.BlockSpec(memory_space=pltpu.HBM)


def place_of():
    row, col = lax.axis_index("row"), lax.axis_index("col")
    return row, col, lax.rem(col, CORES), col // CORES


def order_kernel(own, n_chip, pairs, count_ref, rows_ref, cols_ref, order_ref):
    slots = rows_ref.shape[-1]
    bins = CORES * n_chip * own
    bf16, f32 = jnp.bfloat16, jnp.float32
    _, _, core, chip = place_of()

    def iota(shape, dim):
        return lax.broadcasted_iota(jnp.int32, shape, dim)

    def hot(mask):
        return jnp.where(mask, 1.0, 0.0).astype(bf16)

    def mul(x, y):
        return jnp.dot(x.astype(bf16), y.astype(bf16), preferred_element_type=f32)

    slot = iota((1, slots), 1)
    alive = slot < count_ref[0, 0]
    rows = jnp.where(alive, rows_ref[...], 0)
    cols = jnp.where(alive, cols_ref[...], 0)
    owner = rows // own
    target = owner // CORES
    other = jnp.where(lax.rem(owner, CORES) == core, 0, 1)
    rank = jnp.where(chip < n_chip // 2, n_chip - 1 - target, target)
    local = rank * own + lax.rem(rows, own)
    bin_of = jnp.where(alive, other * n_chip * own + local, -1)
    belongs = bin_of == iota((bins, slots), 0)
    ranks = mul(hot(belongs), hot(iota((slots, slots), 0) <= iota((slots, slots), 1)))
    totals = jnp.broadcast_to(ranks[:, slots - 1 :], (bins, TILE)).astype(jnp.int32)
    halves = (totals + 1) // 2
    before = hot(iota((bins, bins), 1) < iota((bins, bins), 0))
    offsets = 32.0 * mul(before, (halves // 32).astype(f32)) + mul(before, (halves % 32).astype(f32))
    spots = jnp.where(belongs, ranks - 1.0 + 2.0 * offsets[:, :1], 0.0)
    spot = jnp.where(alive, jnp.sum(spots, axis=0, keepdims=True), -1.0)
    odd = jnp.where(alive, spot.astype(jnp.int32) % 2, -1)
    facts = []
    for side in range(2):
        here = odd == side
        facts += [
            jnp.where(here, fact, 0)
            for fact in (slot // 32, slot % 32, jnp.where(here, 1, 0), cols, local)
        ]
    facts = jnp.concatenate(
        [fact.astype(f32) for fact in facts] + [jnp.zeros((EXTRA - len(facts), slots), f32)], axis=0
    )
    pair_of = jnp.broadcast_to(spot, (TILE, slots)).T.astype(jnp.int32) >> 1
    for start in range(0, pairs, TILE):
        found = mul(facts, hot(pair_of == iota((slots, TILE), 1) + start)).astype(jnp.int32)
        places = [32 * found[i : i + 1] + found[i + 1 : i + 2] + found[i + 2 : i + 3] for i in (0, 5)]
        row, cols = found[4:5], (found[3:4], found[8:9])
        order_ref[:, start : start + TILE] = (row << (2 * SLOT_BITS)) + (places[1] << SLOT_BITS) + places[0]
        order_ref[:, pairs + start : pairs + start + TILE] = (
            (cols[1] << (2 * CODE_BITS)) + (cols[0] << CODE_BITS) + row
        )
    end = jnp.sum(halves.astype(f32), axis=0, keepdims=True).astype(jnp.int32)
    order_ref[:, 2 * pairs : 2 * pairs + bins] = offsets.T[0:1, :].astype(jnp.int32)
    order_ref[:, 2 * pairs + bins : 2 * pairs + bins + TILE] = end


def spans_of(order_ref, pairs, half_bins, other, first, last):
    base = 2 * pairs + other * half_bins
    return order_ref[0, base], order_ref[0, base + first], order_ref[0, base + last]


def lists_of(orders, total_pairs, half_bins, first, last):
    pairs = BUILD_UNROLL // 2
    spans, start = [], 0
    for other, order_ref in enumerate(orders):
        low, begin, end = spans_of(order_ref, total_pairs, half_bins, other, first, last)
        spans.append((start - low, begin, end))
        high = spans_of(order_ref, total_pairs, half_bins, other, 0, half_bins)[2]
        start = start + (high - low + pairs - 1) // pairs * pairs
    return spans, start // pairs


def build_kernel(
    half_bins, total_pairs, order_a, order_b, edges_a, edges_b, kept_ref, store_ref, degree_ref,
    edges_ref, made, degree_acc, sem, edge_sem
):
    loads = [
        pltpu.make_async_copy(source, edges_ref.at[i], edge_sem.at[i])
        for i, source in enumerate((edges_a, edges_b))
    ]
    for load in loads:
        load.start()
    degree_acc[...] = jnp.zeros_like(degree_acc)
    pairs = BUILD_UNROLL // 2
    (span_a, span_b), turns = lists_of((order_a, order_b), total_pairs, half_bins, 0, half_bins)
    turns_a = (span_b[0] + span_b[1]) // pairs
    kept_turns = jnp.minimum(turns, KEPT_PAIRS // pairs)
    mask = 2**SLOT_BITS - 1
    cells = [
        (lax.broadcasted_iota(jnp.int32, (HOT_ROWS, TILE), 0) + start).astype(jnp.int8)
        for start in range(0, TILE, HOT_ROWS)
    ]

    def hot(ids):
        ids = jnp.broadcast_to(ids, (HOT_ROWS, TILE)).astype(jnp.int8)
        return jnp.concatenate(
            [jnp.where(ids == cell, HOT(1), HOT(0)) for cell in cells], axis=0
        )

    def fill(turn, target):
        mine = turn < turns_a
        other = jnp.where(mine, 0, 1)
        high = jnp.where(mine, span_a[2], span_b[2])
        low = turn * pairs - jnp.where(mine, 0, span_b[0])
        for pair in range(pairs):
            counts = []
            base = low + pair
            code = jnp.where(mine, order_a[0, base], order_b[0, base])
            live = jnp.where(base < high, code, 0)
            for half in range(2):
                slot = ((live >> (half * SLOT_BITS)) & mask) - 1
                safe = jnp.maximum(slot, 0)
                dst = jnp.where(slot >= 0, edges_ref[other, 0, pl.ds(safe, 1), :], -1)
                src = edges_ref[other, 1, pl.ds(safe, 1), :]
                both = lax.dot_general(
                    hot(src), hot(dst), (((1,), (1,)), ((), ())), preferred_element_type=jnp.float32
                )
                target[pair, half * TILE : (half + 1) * TILE] = both.astype(jnp.bfloat16)
                counts.append(jnp.sum(both.reshape(TILE // 8, 8, TILE), axis=0))
            degree_acc[live >> (2 * SLOT_BITS)] += counts[0] + counts[1]

    def keep(turn, carry):
        fill(turn, kept_ref.at[pl.ds(turn * pairs, pairs)])
        return carry

    for load in loads:
        load.wait()
    lax.fori_loop(0, kept_turns, keep, 0)

    def out_copy(turn):
        side = lax.rem(turn, BUILD_SLOTS)
        return pltpu.make_async_copy(
            made.at[side], store_ref.at[pl.ds(turn * pairs, pairs)], sem.at[side]
        )

    def spill(turn, carry):
        @pl.when(turn >= kept_turns + BUILD_SLOTS)
        def _():
            out_copy(turn - BUILD_SLOTS).wait()

        fill(turn, made.at[lax.rem(turn, BUILD_SLOTS)])
        out_copy(turn).start()
        return carry

    lax.fori_loop(kept_turns, turns, spill, 0)
    for back in range(BUILD_SLOTS, 0, -1):

        @pl.when(turns - back >= kept_turns)
        def _():
            out_copy(turns - back).wait()

    degree_ref[...] = jnp.sum(degree_acc[...], axis=1)


def apply_kernel(half_bins, total_pairs, first_row, orders, kept_ref, store_ref, source_ref, out_ref, held, acc, sem):
    acc[...] = jnp.zeros_like(acc)
    rows = out_ref.shape[0]
    code_mask = 2**CODE_BITS - 1
    spans, _ = lists_of(orders, total_pairs, half_bins, first_row, first_row + rows)

    for other, order_ref in enumerate(orders):
        shift, low, high = spans[other]
        offset = other * source_ref.shape[0] // 2
        edge = jnp.minimum(high, KEPT_PAIRS - shift)
        late = jnp.maximum(low, KEPT_PAIRS - shift)

        def add(base, end, tile):
            code = order_ref[0, total_pairs + base]
            left = (code >> CODE_BITS) & code_mask
            right = code >> (2 * CODE_BITS)
            sources = jnp.concatenate(
                [source_ref[offset + left], source_ref[offset + right]], axis=1
            )
            place = jnp.where(base < end, (code & code_mask) - first_row, rows)
            acc[place] += jnp.dot(sources, tile, preferred_element_type=jnp.float32)

        def visit(turn, carry):
            for pair in range(APPLY_UNROLL // 2):
                base = low + turn * (APPLY_UNROLL // 2) + pair
                add(base, edge, kept_ref[base + shift])
            return carry

        lax.fori_loop(0, (edge - low + APPLY_UNROLL // 2 - 1) // (APPLY_UNROLL // 2), visit, 0)

        def visit_late(turn, carry):
            first = late + turn * LATE_PAIRS
            copy = pltpu.make_async_copy(
                store_ref.at[pl.ds(first + shift, LATE_PAIRS)], held, sem
            )
            copy.start()
            copy.wait()
            for pair in range(LATE_PAIRS):
                add(first + pair, high, held[pair])
            return carry

        lax.fori_loop(0, (high - late + LATE_PAIRS - 1) // LATE_PAIRS, visit_late, 0)
    out_ref[...] = acc[:rows].astype(jnp.bfloat16)


def greet(targets):
    barrier = pltpu.get_barrier_semaphore()
    for target in targets:
        pl.semaphore_signal(barrier, inc=1, device_id=target, device_id_type=MESH_ID)
    pl.semaphore_wait(barrier, len(targets))


def row_peers(n_row, side=0):
    row, col, core, chip = place_of()
    if side:
        col = chip * CORES + 1 - core
    return [(lax.rem(row + d, n_row), col) for d in range(1, n_row)]


def sibling_peers(n_col):
    row, col, _, _ = place_of()
    return [(row, lax.rem(col + CORES * d, n_col)) for d in range(1, n_col // CORES)]


def partner_of():
    row, col, core, chip = place_of()
    return (row, chip * CORES + 1 - core)


def remote(src, dst, send_sem, recv_sem, target):
    return pltpu.make_async_remote_copy(
        src_ref=src,
        dst_ref=dst,
        send_sem=send_sem,
        recv_sem=recv_sem,
        device_id=target,
        device_id_type=MESH_ID,
    )


def send(*args):
    copy = remote(*args)
    copy.start()
    return copy


def start_kernel(n_row, n_col, part, *refs):
    blocks = refs[:n_row]
    gathered_ref, root_ref, taken, theirs, roots = refs[n_row : n_row + 5]
    deg_send, deg_recv, near_send, near_recv, root_send, root_recv = refs[n_row + 5 :]
    row, col, core, chip = place_of()
    n_chip = n_col // CORES
    own = root_ref.shape[0]
    partner = partner_of()
    siblings = sibling_peers(n_col)
    mine, cross = row_peers(n_row), row_peers(n_row, 1)
    greet(siblings + mine + cross + [partner])
    copies = []
    low_half = chip < n_chip // 2
    for d, target in enumerate(siblings):
        rank = target[1] // CORES
        start = jnp.where(low_half, n_chip - 1 - rank, rank) * own
        copies.append(
            send(
                part.at[pl.ds(pl.multiple_of(start, own), own)],
                taken.at[d],
                deg_send.at[d],
                deg_recv.at[d],
                target,
            )
        )
    near = []
    for d in range(n_row):
        near.append(send(blocks[d], theirs.at[d], near_send.at[d], near_recv.at[d], partner))
    mine_rank = jnp.where(low_half, n_chip - 1 - chip, chip)
    def start_of(side, d):
        return side * n_row * own + lax.rem(row + n_row - d, n_row) * own

    def turn(side, d, source):
        for tile in range(own):
            block = source[tile * TILE : (tile + 1) * TILE, :].astype(jnp.float32).T
            gathered_ref[start_of(side, d) + tile] = block.astype(jnp.bfloat16)

    for d in range(n_row):
        turn(0, d, blocks[d])
    degree = part[pl.ds(pl.multiple_of(mine_rank * own, own), own), :]
    for d, copy in enumerate(copies):
        copy.wait_recv()
        degree = degree + taken[d]
    root = lax.rsqrt(1.0 + degree)
    root_ref[...] = root
    roots[0, 0] = root
    root_copies = []
    for side, targets in ((0, mine), (1, [partner] + cross)):
        for d, target in enumerate(targets):
            d += 1 - side
            root_copies.append(
                send(roots.at[0, 0], roots.at[side, d], root_send.at[side, d], root_recv.at[side, d], target)
            )

    def scale(side, d, root):
        for tile in range(own):
            place = start_of(side, d) + tile
            gathered_ref[place] = (
                gathered_ref[place].astype(jnp.float32) * root[tile : tile + 1, :]
            ).astype(jnp.bfloat16)

    for d in range(n_row):
        near[d].wait_recv()
        turn(1, d, theirs.at[d])
    scale(0, 0, root)
    for copy in root_copies:
        copy.wait_recv()
    for side in range(2):
        for d in range(1 - side, n_row):
            scale(side, d, roots[side, d])
    for copy in copies + near + root_copies:
        copy.wait_send()


def sum_kernel(n_row, n_col, spread, *refs):
    parts, given, refs = refs[: EARLY + 1], refs[EARLY + 1 : 2 * EARLY + 1], refs[2 * EARLY + 1 :]
    if spread:
        root_ref, hop_ref, gathered_ref, comes, goes, *sems = refs
        send_sem, recv_sem, row_send, row_recv, near_send, near_recv = sems
    else:
        root_ref, hop_ref, comes, goes, send_sem, recv_sem = refs
    row, col, core, chip = place_of()
    n_chip = n_col // CORES
    own = root_ref.shape[0]
    size = own // PIECES
    partner = partner_of()
    up = (row, lax.rem(col + CORES, n_col))
    down = (row, lax.rem(col + n_col - CORES, n_col))
    mine = row_peers(n_row)
    greet([up, down] + ([partner] + mine if spread else []))
    last = n_chip - 1
    low_half = chip < n_chip // 2
    early = jnp.where(low_half, 0, 1)
    depth = jnp.where(low_half, chip, last - chip)

    def block(rank, piece):
        if rank < EARLY:
            return parts[rank].at[piece * size : (piece + 1) * size]
        start = (rank - EARLY) * own + piece * size
        return parts[EARLY].at[start : start + size]

    def hop_copy(way, k, piece, source=None):
        return remote(
            goes.at[way, k, piece] if source is None else source,
            comes.at[way, k, piece],
            send_sem.at[way, k, piece],
            recv_sem.at[way, k, piece],
            (row, lax.rem(col + jnp.where(way == 0, CORES, n_col - CORES), n_col)),
        )

    flow = [(k, piece) for k in range(last) for piece in range(PIECES)]
    timed = [(i, 0, *f) for i, f in enumerate(flow)]
    timed += [(i + RELAY_LAG, 1, *f) for i, f in enumerate(flow) if f[0] < n_chip // 2 - 1]

    def steps():
        for _, late, k, piece in sorted(timed):
            way = 1 - early if late else early
            ahead = k < (depth if late else last - depth)
            yield k, piece, late, way, ahead

    for k, piece, late, way, ahead in steps():
        source = block(last - k if late else k, piece)

        def relay(arrived):
            goes[way, k, piece] = (
                source[...].astype(jnp.float32) + arrived.astype(jnp.float32)
            ).astype(jnp.bfloat16)
            hop_copy(way, k, piece).start()

        def relay_waited():
            hop_copy(way, k, piece).wait_recv()
            relay(comes[way, k, piece])

        if late:
            pl.when(ahead)(relay_waited)
        elif k >= EARLY:
            pl.when(ahead & (depth == 0))(lambda: hop_copy(way, k, piece, source).start())
            pl.when(ahead & (depth > 0))(relay_waited)
        else:
            pl.when(ahead & (depth == 1))(
                lambda: relay(given[k][piece * size : (piece + 1) * size])
            )
            pl.when(ahead & (depth > 1))(relay_waited)

    row_copies, near_copies = {}, {}
    for piece in range(PIECES):
        early_k = jnp.minimum(last - depth, last - 1)

        @pl.when(depth > 0)
        def _():
            hop_copy(early, early_k, piece).wait_recv()

        hop_copy(1 - early, depth, piece).wait_recv()
        start = pl.multiple_of((last - depth - EARLY) * own, own) + piece * size
        total = parts[EARLY][pl.ds(start, size)].astype(jnp.float32)
        near = comes[early, early_k, piece].astype(jnp.float32)
        total = total + jnp.where(depth > 0, near, 0.0)
        total = total + comes[1 - early, depth, piece].astype(jnp.float32)
        roots = [root_ref[piece * size + tile : piece * size + tile + 1, :] for tile in range(size)]
        if spread:
            start = row * own + piece * size
            for tile in range(size):
                gathered_ref[start + tile] = (total[tile] * (roots[tile] * roots[tile])).astype(
                    jnp.bfloat16
                )
            for d, target in enumerate(mine):
                place = gathered_ref.at[pl.ds(start, size)]
                row_copies[piece, d] = send(
                    place, place, row_send.at[piece, d], row_recv.at[piece, d], target
                )
            near_copies[piece, 0] = send(
                gathered_ref.at[pl.ds(start, size)],
                gathered_ref.at[pl.ds(n_row * own + start, size)],
                near_send.at[piece, 0],
                near_recv.at[piece, 0],
                partner,
            )
        for tile in range(size):
            place = (piece * size + tile) * TILE
            hop_ref[place : place + TILE, :] = (total[tile] * roots[tile]).T.astype(jnp.bfloat16)
    for (piece, d), copy in row_copies.items():
        copy.wait_recv()
        start = lax.rem(row + n_row - d - 1, n_row) * own + piece * size
        near_copies[piece, d + 1] = send(
            gathered_ref.at[pl.ds(start, size)],
            gathered_ref.at[pl.ds(n_row * own + start, size)],
            near_send.at[piece, d + 1],
            near_recv.at[piece, d + 1],
            partner,
        )
    for copy in near_copies.values():
        copy.wait_recv()
    for copy in list(row_copies.values()) + list(near_copies.values()):
        copy.wait_send()
    for k, piece, late, way, ahead in steps():
        if not late and k < EARLY:
            ahead = ahead & (depth > 0)
        pl.when(ahead)(lambda: hop_copy(way, k, piece).wait_send())


def sems(*shape):
    return pltpu.SemaphoreType.DMA(shape)


def comm_params(ident, scratch):
    return pltpu.CompilerParams(
        collective_id=ident, has_side_effects=True, vmem_limit_bytes=scratch + 2**20
    )


def full_params():
    return pltpu.CompilerParams(vmem_limit_bytes=67043328)


def plain_params(scratch):
    return pltpu.CompilerParams(vmem_limit_bytes=scratch + 2**20)


def local(features, tile_rows, tile_cols, edge_lists, tile_counts):
    node_count, feat_width = features.shape
    n_row, n_col = lax.axis_size("row"), lax.axis_size("col")
    n_chip = n_col // CORES
    own = node_count // TILE
    half_tiles = own * n_chip
    source_tiles = own * n_row
    slots = tile_rows.shape[-1]
    bf16, f32 = jnp.bfloat16, jnp.float32
    tile_bytes = feat_width * TILE * 2
    spare = max(BUILD_UNROLL, APPLY_UNROLL)
    pairs = -(-(slots + CORES * half_tiles + spare) // (2 * TILE)) * TILE
    swap = [(i, i + 1 - 2 * (i % CORES)) for i in range(n_col)]
    edges = edge_lists.reshape(2, slots, TILE)

    blocks = [features] + [
        lax.ppermute(features, "row", [(i, (i + d) % n_row) for i in range(n_row)])
        for d in range(1, n_row)
    ]
    edges_b = lax.ppermute(edges, "col", swap)
    codes = 2 * pairs + -(-(CORES * half_tiles) // TILE) * TILE + TILE
    order = pl.pallas_call(
        functools.partial(order_kernel, own, n_chip, pairs),
        out_shape=jax.ShapeDtypeStruct((1, codes), jnp.int32),
        in_specs=[SMEM_SPEC] + [VMEM_SPEC] * 2,
        out_specs=VMEM_SPEC,
        compiler_params=plain_params(16 * 2**20),
        cost_estimate=pl.CostEstimate(flops=10**10, bytes_accessed=0, transcendentals=0),
        name="order",
    )(tile_counts, tile_rows[0], tile_cols[0])
    order_b = lax.ppermute(order, "col", swap)

    kept, store, degree = pl.pallas_call(
        functools.partial(build_kernel, half_tiles, pairs),
        in_specs=[SMEM_SPEC] * 2 + [HBM_SPEC] * 2,
        out_specs=[VMEM_SPEC, ANY_SPEC, VMEM_SPEC],
        scratch_shapes=[
            pltpu.VMEM((2, 2, slots, TILE), jnp.int32),
            pltpu.VMEM((BUILD_SLOTS, BUILD_UNROLL // 2, 2 * TILE, TILE), bf16),
            pltpu.VMEM((half_tiles, 8, TILE), f32),
            sems(BUILD_SLOTS),
            sems(2),
        ],
        out_shape=[
            jax.ShapeDtypeStruct((KEPT_PAIRS + APPLY_UNROLL // 2, 2 * TILE, TILE), bf16),
            jax.ShapeDtypeStruct((2 * pairs, 2 * TILE, TILE), bf16),
            jax.ShapeDtypeStruct((half_tiles, TILE), f32),
        ],
        compiler_params=plain_params(4 * slots * TILE * 4 + BUILD_UNROLL * TILE * TILE * 2),
        name="build",
    )(order, order_b, edges, edges_b)

    gathered_type = jax.ShapeDtypeStruct((CORES * source_tiles, feat_width, TILE), bf16)
    gathered, root = pl.pallas_call(
        functools.partial(start_kernel, n_row, n_col),
        out_shape=[gathered_type, jax.ShapeDtypeStruct((own, TILE), f32)],
        in_specs=[VMEM_SPEC] * (1 + n_row),
        out_specs=[VMEM_SPEC] * 2,
        scratch_shapes=[
            pltpu.VMEM((n_chip - 1, own, TILE), f32),
            pltpu.VMEM((n_row, node_count, feat_width), bf16),
            pltpu.VMEM((2, n_row, own, TILE), f32),
            sems(n_chip - 1),
            sems(n_chip - 1),
            sems(n_row),
            sems(n_row),
            sems(2, n_row),
            sems(2, n_row),
        ],
        compiler_params=comm_params(0, n_row * own * tile_bytes),
        name="start",
    )(degree, *blocks)

    def apply(sources, ranks, after, hop=None):
        rows = len(ranks) * own
        hops = [] if hop is None else [hop]

        def body(order_a, order_b, kept, store, sources, after, *refs):
            if hops:
                hop_ref, out_ref, hop_out, *scratch, hop_sem = refs
                copy = pltpu.make_async_copy(hop_ref, hop_out, hop_sem)
                copy.start()
            else:
                out_ref, *scratch = refs
            apply_kernel(
                half_tiles,
                pairs,
                ranks[0] * own,
                (order_a, order_b),
                kept,
                store,
                sources,
                out_ref,
                *scratch,
            )
            if hops:
                copy.wait()

        return pl.pallas_call(
            body,
            in_specs=[SMEM_SPEC] * 2
            + [VMEM_SPEC, ANY_SPEC] * 2
            + [VMEM_SPEC] * len(hops),
            out_specs=[VMEM_SPEC] + [ANY_SPEC] * len(hops),
            scratch_shapes=[
                pltpu.VMEM((LATE_PAIRS, 2 * TILE, TILE), bf16),
                pltpu.VMEM((rows + 1, feat_width, TILE), f32),
                pltpu.SemaphoreType.DMA,
            ]
            + [pltpu.SemaphoreType.DMA] * len(hops),
            out_shape=[jax.ShapeDtypeStruct((rows, feat_width, TILE), bf16)]
            + [jax.ShapeDtypeStruct(hop.shape, hop.dtype) for hop in hops],
            compiler_params=plain_params((2 * rows + 2 + 2 * LATE_PAIRS) * tile_bytes),
            cost_estimate=pl.CostEstimate(flops=10**10, bytes_accessed=0, transcendentals=0),
            name="apply",
        )(order, order_b, kept, store, sources, after, *hops)

    ends = [
        (a * CORES + core, b * CORES + core)
        for a, b in ((0, 1), (n_chip - 1, n_chip - 2))
        for core in range(CORES)
    ]

    def apply_all(sources, hop=None):
        parts, given, after = [], [], sources
        for rank in range(EARLY):
            (part,) = apply(sources, [rank], after)
            parts.append(part)
            given.append(lax.ppermute(part, "col", ends))
            after = part
        part, *hops = apply(sources, list(range(EARLY, n_chip)), after, hop)
        return parts + [part] + given, *hops

    def collect(parts, spread):
        size = own // PIECES
        outs = [jax.ShapeDtypeStruct((node_count, feat_width), bf16)]
        semaphores = [sems(2, n_chip - 1, PIECES)] * 2
        if spread:
            outs.append(gathered_type)
            semaphores += [sems(PIECES, n_row - 1)] * 2 + [sems(PIECES, n_row)] * 2
        return pl.pallas_call(
            functools.partial(sum_kernel, n_row, n_col, spread),
            out_shape=outs,
            in_specs=[VMEM_SPEC] * (len(parts) + 1),
            out_specs=[VMEM_SPEC] * len(outs),
            scratch_shapes=[pltpu.VMEM((2, n_chip - 1, PIECES, size, feat_width, TILE), bf16)] * 2
            + semaphores,
            compiler_params=comm_params(
                1 if spread else 2, 4 * (n_chip - 1) * own * tile_bytes
            ),
            name="spread" if spread else "finish",
        )(*parts, root)

    (parts,) = apply_all(gathered)
    hop_one, gathered = collect(parts, True)
    parts, hop_one = apply_all(gathered, hop_one)
    (hop_two,) = collect(parts, False)
    return (hop_one, hop_two)


def solution(mesh):
    placed = (
        P(("row", "col"), None),
        P("row", "col", None),
        P("row", "col", None),
        P(None, "row", "col", None, None),
        P("row", "col"),
    )
    return jax.shard_map(
        local,
        mesh=mesh,
        in_specs=placed,
        out_specs=(P(("row", "col"), None), P(("row", "col"), None)),
        check_vma=False,
    )
```
